256 devices in a mesh: rows: 256 (over y, x, z, core).
Axes of the slice: x: 4, y: 4, z: 8, core: 2. Of those that a mesh axis runs over, the one named last changes fastest.
Arguments:
- factor: bfloat16 [2097152, 256], P('rows')
- cand_weights: bfloat16 [524288, 1024], P('rows'), may hold values from -2 to 2
- cand_block: int32 [1024], replicated, may hold values from 0 to 3
- noise: float32 [1024], replicated, may hold values from 0.3 to 3
- chosen: int32 [2], replicated, may hold values from 0 to 1023
Outputs:
- scores: float32 [2, 1024], P(None, 'rows')
- updates: float32 [2, 2097152], P(None, 'rows')
The draws below stay inside these ranges and needn't reach their ends.
All inputs are finite; a program needn't handle non-finite values.
Results may differ from the reference program's by a relative error of at most 0.00055.
Values sent between devices are 32-bit elements; how exact they have to be, the bound alone decides.
No kernel may reach another device: no remote copies, remote signals or barrier semaphores. Data moves between devices by JAX's collectives and lax.ppermute only.
A program may use at most 128 MiB of HBM per device.

```python
import math
import jax
import jax.numpy as jnp
from jax import lax

R = 256
NCAND = 1024
NB = 4
ROWS_DEV = 8192
N = 2097152


def factor_float(key):
    keys = jax.random.split(jax.random.fold_in(key, 11), 3)
    rowpos = jnp.arange(N, dtype=jnp.float32)
    rowscale = 1.0 + 2.0 * rowpos / N
    colscale = jnp.exp(jax.random.uniform(keys[1], (R,), jnp.float32, math.log(0.3), math.log(3.0)))
    mixing = jnp.eye(R, dtype=jnp.float32) + 0.6 * jax.random.normal(keys[2], (R, R), jnp.float32) / math.sqrt(R)
    base = jax.random.normal(keys[0], (N, R), jnp.float32)
    mixed = jnp.dot(base * colscale[None, :], mixing, precision=lax.Precision.HIGHEST)
    return mixed * rowscale[:, None] / math.sqrt(N)


def block_ids(key):
    return jax.random.randint(jax.random.fold_in(key, 23), (NCAND,), 0, NB, dtype=jnp.int32)


def draw_factor(key, part):
    return factor_float(key).astype(jnp.bfloat16)


def draw_cand_block(key, part):
    return block_ids(key)


def draw_cand_weights(key, part):
    keys = jax.random.split(jax.random.fold_in(key, 37), 6)
    grouped = factor_float(key).reshape(N // NB, NB, R)
    blocks = block_ids(key)
    shared = jax.random.normal(keys[0], (R,), jnp.float32)
    loads = jax.random.normal(keys[1], (NCAND,), jnp.float32)
    own = jax.random.normal(keys[2], (R, NCAND), jnp.float32)
    mixing = shared[:, None] * loads[None, :] + own
    coherent = jnp.zeros((N // NB, NCAND), jnp.float32)
    for block in range(NB):
        seen = jnp.dot(grouped[:, block, :], mixing, precision=lax.Precision.HIGHEST)
        coherent = coherent + jnp.where(blocks[None, :] == block, seen, 0.0)
    coherent = coherent / jnp.sqrt(jnp.sum(coherent * coherent, axis=0, keepdims=True))
    noisy = jax.random.normal(keys[3], (N // NB, NCAND), jnp.float32) / math.sqrt(N // NB)
    raw = coherent + 0.5 * noisy
    devices = N // ROWS_DEV
    row_owner = jnp.arange(N // NB, dtype=jnp.int32) // (ROWS_DEV // NB)
    cand_owner = jnp.arange(NCAND, dtype=jnp.int32) // (NCAND // devices)
    pairing = jax.random.permutation(keys[4], devices)
    boost = jnp.where(pairing[row_owner][:, None] == cand_owner[None, :], 4.0, 1.0)
    raw = raw * boost
    colnorm = jnp.exp(jax.random.uniform(keys[5], (NCAND,), jnp.float32, math.log(0.5), math.log(2.0)))
    raw = raw * (colnorm / jnp.sqrt(jnp.sum(raw * raw, axis=0)))[None, :]
    return raw.astype(jnp.bfloat16)


def setup_inputs(seed: int = 0) -> dict:
    streams_of = jax.random.split(jax.random.key(seed), 6)
    return {
        "factor": draw_factor(jax.random.fold_in(streams_of[5], 71), 0),
        "cand_weights": draw_cand_weights(jax.random.fold_in(streams_of[5], 71), 0),
        "cand_block": draw_cand_block(jax.random.fold_in(streams_of[5], 71), 0),
        "noise": jnp.clip(jnp.exp(jax.random.uniform(streams_of[3], (NCAND,), jnp.float32, math.log(0.3), math.log(3.0))), 0.3, 3.0),
        "chosen": jax.random.randint(streams_of[4], (2,), 0, NCAND).astype(jnp.int32),
    }


def posterior_terms(proj, sq, cross, noise_rows, gram, psel, ssel, noise_sel, solve):
    highest = lax.Precision.HIGHEST
    coeffs = solve(proj)
    coeff_sel = solve(psel)
    kcoef = jnp.dot(coeffs, gram, precision=highest)
    proj_a = lax.optimization_barrier(jnp.sum(proj * coeffs, axis=1))
    quad = lax.optimization_barrier(jnp.sum(coeffs * kcoef, axis=1))
    qval = sq - proj_a
    normsq = sq - 2.0 * proj_a + quad
    first_p, second_p = (psel[0], psel[1])
    first_a, second_a = (coeff_sel[0], coeff_sel[1])
    first_pa = jnp.dot(first_p, first_a, precision=highest)
    first_q = ssel[0] - first_pa
    big = ssel[0] - 2.0 * first_pa + jnp.dot(first_a, jnp.dot(gram, first_a, precision=highest), precision=highest)
    dfirst = noise_sel[0] + first_q
    inner = cross - jnp.dot(coeffs, first_p, precision=highest)
    along = inner - jnp.dot(proj, first_a, precision=highest) + jnp.dot(kcoef, first_a, precision=highest)
    qnext = qval - inner * inner / dfirst
    nnext = normsq - 2.0 * inner * along / dfirst + inner * inner * big / (dfirst * dfirst)
    scores = jnp.stack([normsq / (noise_rows + qval), nnext / (noise_rows + qnext)])
    inner_two = ssel[2] - jnp.dot(first_p, second_a, precision=highest)
    second_q = ssel[1] - jnp.dot(second_p, second_a, precision=highest)
    dsecond = noise_sel[1] + second_q - inner_two * inner_two / dfirst
    return (scores, coeff_sel, dfirst, dsecond, inner_two)

def reference(factor, cand_weights, cand_block, noise, chosen):
    highest = lax.Precision.HIGHEST
    grouped = factor.reshape(N // NB, NB, R)
    onehot = (cand_block[:, None] == jnp.arange(NB, dtype=jnp.int32)[None, :]).astype(jnp.float32)
    proj = jnp.zeros((NCAND, R), jnp.float32)
    for block in range(NB):
        part_proj = jnp.einsum('ic,ir->cr', cand_weights.astype(jnp.float32), grouped[:, block, :].astype(jnp.float32), preferred_element_type=jnp.float32)
        proj = proj + onehot[:, block:block + 1] * part_proj
    gram = jnp.einsum('ir,is->rs', factor.astype(jnp.float32), factor.astype(jnp.float32), preferred_element_type=jnp.float32)
    wfloat = cand_weights.astype(jnp.float32)
    sq = lax.optimization_barrier(jnp.sum(wfloat * wfloat, axis=0))
    first = chosen[0]
    second = chosen[1]
    same = (cand_block == cand_block[first]).astype(jnp.float32)
    cross = jnp.dot(cand_weights.T.astype(jnp.float32), cand_weights[:, first].astype(jnp.float32), preferred_element_type=jnp.float32) * same
    psel = jnp.stack([proj[first], proj[second]])
    ssel = jnp.stack([sq[first], sq[second], cross[second]])
    noise_sel = jnp.stack([noise[first], noise[second]])
    system = jnp.eye(R, dtype=jnp.float32) + gram

    def solve(rhs):
        return jnp.linalg.solve(system, rhs.T).T
    scores, coeff_sel, dfirst, dsecond, inner_two = posterior_terms(proj, sq, cross, noise, gram, psel, ssel, noise_sel, solve)
    wsel = jnp.stack([wfloat[:, first], wfloat[:, second]], axis=1)
    sel_onehot = jnp.stack([onehot[first], onehot[second]], axis=1)
    dense = (wsel[:, None, :] * sel_onehot[None, :, :]).reshape(N, 2)
    applied = jnp.dot(factor.astype(jnp.float32), coeff_sel.T, precision=highest)
    first_vec = dense[:, 0] - applied[:, 0]
    second_vec = dense[:, 1] - applied[:, 1] - first_vec * inner_two / dfirst
    updates = jnp.stack([first_vec / jnp.sqrt(dfirst), second_vec / jnp.sqrt(dsecond)])
    return (scores, updates)
```

```python
import jax
import jax.numpy as jnp
from jax import lax
from jax.experimental import pallas as pl
from jax.experimental.pallas import tpu as pltpu
from jax.sharding import Mesh
from jax.sharding import PartitionSpec as P

NB = 4
R = 256
NCAND = 1024
LANES = 128
NYX = 16
NZ = 8
SLOTS = NZ + 2
STEPS = 4
ROWS = ("rows_0", "rows_1", "rows_2", "rows_3")
YX = ("rows_0", "rows_1")
HIGHEST = lax.Precision.HIGHEST


def iota(shape, dim):
    return lax.broadcasted_iota(jnp.int32, shape, dim)


def matmul(a, b, dims=((1,), (0,)), precision=None):
    return lax.dot_general(
        a, b, (dims, ((), ())), preferred_element_type=jnp.float32, precision=precision
    )


def local_kernel(
    chosen, blocks, core, fac, wts, block_row, mine, theirs, dense,
    fwide, acc, gram, sq8, cross8, masks, wsel, pay,
):
    step = pl.program_id(0)
    wrows = wts.shape[0]
    first, second = chosen[0], chosen[1]

    @pl.when(step == 0)
    def _():
        acc[...] = jnp.zeros_like(acc)
        gram[...] = jnp.zeros_like(gram)
        sq8[...] = jnp.zeros_like(sq8)
        cross8[...] = jnp.zeros_like(cross8)
        pay[:, :, NZ:, :, :] = jnp.zeros((2, NYX, 2, 8, LANES), jnp.float32)
        column = jnp.broadcast_to(block_row[...], (LANES, NCAND)).T
        for b in range(NB):
            masks[b] = jnp.where(column == float(b), 1.0, 0.0).astype(jnp.bfloat16)

    w = wts[...]
    for h in range(2):
        fwide[h] = fac[:, LANES * h : LANES * (h + 1)].astype(jnp.float32)
    turned = w.T
    total = acc[...]
    gsum = gram[...]
    for b in range(NB):
        fb = jnp.concatenate(
            [fwide[h, pl.ds(b, wrows, stride=NB), :] for h in range(2)], axis=1
        ).astype(jnp.bfloat16)
        mask = masks[b]
        seen = jnp.concatenate(
            [turned[:, LANES * q : LANES * (q + 1)] * mask for q in range(wrows // LANES)], axis=1
        )
        total = total + matmul(seen, fb)
        gsum = gsum + matmul(fb, fb, ((0,), (0,)))
    acc[...] = total
    gram[...] = gsum
    wf = w.astype(jnp.float32)
    sq8[...] += jnp.sum((wf * wf).reshape(wrows // 8, 8, NCAND), axis=0)
    rows = iota((16, LANES), 0)
    lanes = iota((16, LANES), 1)
    picked = jnp.zeros((16, wrows), jnp.float32)
    for row, cand in ((0, first), (1, second)):
        base = pl.multiple_of((cand // LANES) * LANES, LANES)
        hot = jnp.where((rows == row) & (lanes == cand - base), 1.0, 0.0).astype(jnp.bfloat16)
        picked = picked + matmul(hot, wts[:, pl.ds(base, LANES)], ((1,), (1,)))
    cross8[...] += matmul(picked.astype(jnp.bfloat16), w)[:8]
    for q in range(wrows // LANES):
        wsel[step * (wrows // LANES) + q] = picked[:8, LANES * q : LANES * (q + 1)]

    @pl.when(step == STEPS - 1)
    def _():
        proj = acc[...]
        for h in range(2):
            half = proj[:, LANES * h : LANES * (h + 1)]
            pay[h, :, :NZ, :, :] = half.reshape(NYX, NZ, 8, LANES)
        g = gram[...]
        pay[0, :, NZ, :, :] = g[:LANES, :LANES].reshape(NYX, 8, LANES)
        pay[1, :, NZ, :, :] = g[:LANES, LANES:].reshape(NYX, 8, LANES)
        low = g[LANES:, LANES:].reshape(2, NYX // 2, 8, LANES)
        pay[0, : NYX // 2, NZ + 1, :, :] = low[0]
        pay[1, : NYX // 2, NZ + 1, :, :] = low[1]
        for row, cand in ((0, first), (1, second)):
            line = acc[pl.ds(cand, 1), :]
            for h in range(2):
                pay[0, NYX // 2, NZ + 1, 2 * row + h : 2 * row + h + 1, :] = line[
                    :, LANES * h : LANES * (h + 1)
                ]
        sq = jnp.sum(sq8[...], axis=0, keepdims=True)
        same = block_row[...] == blocks[first].astype(jnp.float32)
        cross = jnp.where(same, cross8[0:1, :], 0.0)
        for q in range(NCAND // LANES):
            part = slice(LANES * q, LANES * (q + 1))
            pay[1, NYX // 2, NZ + 1, q : q + 1, :] = sq[:, part]
            pay[1, NYX // 2 + 1, NZ + 1, q : q + 1, :] = cross[:, part]
        mine[...] = pay[core[0]]
        theirs[...] = pay[1 - core[0]]
        wide = LANES * NB
        spread = jnp.where(
            iota((LANES, wide), 0) == iota((LANES, wide), 1) // NB, 1.0, 0.0
        ).astype(jnp.bfloat16)
        groups = wsel.shape[0]
        lines = wsel[...].reshape(groups * 8, LANES).astype(jnp.bfloat16)
        repeated = matmul(lines, spread).reshape(groups, 8, wide)
        row = iota((groups, 8, wide), 1)
        place = iota((groups, 8, wide), 2) % NB
        wanted = jnp.where(row == 0, blocks[first], blocks[second])
        dense[...] = jnp.where(place == wanted, repeated, 0.0)


def local_products(factor, cand_weights, cand_block, chosen, core):
    rows, rank = factor.shape
    wrows = cand_weights.shape[0]
    fstep, wstep = rows // STEPS, wrows // STEPS
    groups = wrows // LANES
    payload = jax.ShapeDtypeStruct((NYX, SLOTS, 8, LANES), jnp.float32)
    fixed4 = pl.BlockSpec((NYX, SLOTS, 8, LANES), lambda i, *_: (0, 0, 0, 0))
    return pl.pallas_call(
        local_kernel,
        grid_spec=pltpu.PrefetchScalarGridSpec(
            num_scalar_prefetch=3,
            grid=(STEPS,),
            in_specs=[
                pl.BlockSpec((fstep, rank), lambda i, *_: (i, 0)),
                pl.BlockSpec((wstep, NCAND), lambda i, *_: (i, 0)),
                pl.BlockSpec((1, NCAND), lambda i, *_: (0, 0)),
            ],
            out_specs=[
                fixed4,
                fixed4,
                pl.BlockSpec((groups, 8, LANES * NB), lambda i, *_: (0, 0, 0)),
            ],
            scratch_shapes=[
                pltpu.VMEM((2, fstep, LANES), jnp.float32),
                pltpu.VMEM((NCAND, rank), jnp.float32),
                pltpu.VMEM((rank, rank), jnp.float32),
                pltpu.VMEM((8, NCAND), jnp.float32),
                pltpu.VMEM((8, NCAND), jnp.float32),
                pltpu.VMEM((NB, NCAND, LANES), jnp.bfloat16),
                pltpu.VMEM((groups, 8, LANES), jnp.float32),
                pltpu.VMEM((2, NYX, SLOTS, 8, LANES), jnp.float32),
            ],
        ),
        out_shape=[payload, payload, jax.ShapeDtypeStruct((groups, 8, LANES * NB), jnp.float32)],
        compiler_params=pltpu.CompilerParams(
            dimension_semantics=("arbitrary",), vmem_limit_bytes=60 * 2**20
        ),
        name="local",
    )(
        chosen,
        cand_block,
        core,
        factor,
        cand_weights,
        cand_block.astype(jnp.float32).reshape(1, NCAND),
    )


def total(x):
    return jnp.sum(jnp.sum(x, axis=1, keepdims=True), axis=0, keepdims=True)


def lane_sum(x):
    return jnp.sum(x, axis=1, keepdims=True)


def finish_kernel(
    chosen, where, gmine, gtheirs, pmine, ptheirs, noise, dense, factor, scores, updates,
    fvmem, m, x, sem,
):
    copy = pltpu.make_async_copy(factor, fvmem, sem)
    copy.start()
    core, chip = where[0], where[1]
    first, second = chosen[0], chosen[1]
    own = core == 0
    a_, b_ = gmine[...], gtheirs[...]
    g0 = jnp.where(own, a_, b_)
    g1 = jnp.where(own, b_, a_)
    half = NYX // 2
    top = g0[:, 0].reshape(LANES, LANES)
    side = g1[:, 0].reshape(LANES, LANES)
    low = jnp.concatenate([g0[:half, 1], g1[:half, 1]], axis=0).reshape(LANES, LANES)
    diag = iota((LANES, LANES), 0) == iota((LANES, LANES), 1)
    m[:LANES, :LANES] = top + jnp.where(diag, 1.0, 0.0)
    m[:LANES, LANES:] = side
    m[LANES:, :LANES] = side.T
    m[LANES:, LANES:] = low + jnp.where(diag, 1.0, 0.0)
    psel, sq, cross = g0[half, 1], g1[half, 1], g1[half + 1, 1]
    p_, q_ = pmine[...], ptheirs[...]
    pown = jnp.concatenate([jnp.where(own, p_, q_), jnp.where(own, q_, p_)], axis=1)
    pj = jnp.concatenate([psel[0:1], psel[1:2]], axis=1)
    pk = jnp.concatenate([psel[2:3], psel[3:4]], axis=1)
    rid = iota((8, R), 0)
    pboth = jnp.where(rid >= 6, 0.0, jnp.where(rid % 2 == 0, pj, pk))
    rhs = jnp.concatenate([pown, pboth], axis=0)

    full = m[...]
    rowmax = jnp.max(jnp.sum(jnp.abs(full), axis=0, keepdims=True))
    bound = jnp.maximum(rowmax, 1.0)
    rho0 = (bound - 1.0) / (bound + 1.0)
    alpha = 2.0 / (bound + 1.0)
    eye = jnp.where(iota((R, R), 0) == iota((R, R), 1), 1.0, 0.0)
    scale0 = 2.0 / (2.0 - rho0 * rho0)
    x[...] = (scale0 * alpha) * (2.0 * eye - alpha * full)
    rho1 = rho0 * rho0 / (2.0 - rho0 * rho0)

    def newton(carry):
        rho, count = carry
        scale = 2.0 / (2.0 - rho * rho)
        now = x[...]
        prod = matmul(m[...], now, precision=HIGHEST)
        x[...] = scale * (2.0 * now - matmul(now, prod, precision=HIGHEST))
        return rho * rho / (2.0 - rho * rho), count + 1

    lax.while_loop(lambda s: (s[0] > 5e-3) & (s[1] < 100), newton, (rho1, jnp.int32(0)))
    inv = x[...]
    a = matmul(rhs, inv, precision=HIGHEST)
    for _ in range(2):
        left = rhs - matmul(a, full, precision=HIGHEST)
        a = a + matmul(left, inv, precision=HIGHEST)

    aown, aboth = a[:8], a[8:]
    aj, ak = aboth[0:1], aboth[1:2]
    rows = iota((8, LANES), 0)
    lanes = iota((8, LANES), 1)
    flat = rows * LANES + lanes
    nz = noise[...]

    def at(tile, cand):
        return total(jnp.where(flat == cand, tile, 0.0))

    def owned(tile):
        line = jnp.sum(jnp.where(rows == chip // NYX, tile, 0.0), axis=0, keepdims=True)
        return lane_sum(jnp.where(lanes == (chip % NYX) * 8 + rows, line, 0.0))

    sqc, crossc, noisec = owned(sq), owned(cross), owned(nz)
    pa = lane_sum(pown * aown)
    aa = lane_sum(aown * aown)
    pja = lane_sum(aown * pj)
    aja = lane_sum(aown * aj)
    q = sqc - pa
    nrm = sqc - 2.0 * pa + (pa - aa)
    paj = lane_sum(pj * aj)
    qj = at(sq, first) - paj
    big = at(sq, first) - 2.0 * paj + (paj - lane_sum(aj * aj))
    d1 = at(nz, first) + qj
    u = crossc - pja
    e = u - aja
    q2 = q - u * u / d1
    nrm2 = nrm - 2.0 * u * e / d1 + u * u * big / (d1 * d1)
    for row, s in ((0, nrm / (noisec + q)), (1, nrm2 / (noisec + q2))):
        line = jnp.sum(jnp.where(rows == lanes + 4 * core, s, 0.0), axis=0, keepdims=True)
        scores[row : row + 1, :] = line[:, :4]
    uk = at(cross, second) - lane_sum(pj * ak)
    qk = at(sq, second) - lane_sum(pk * ak)
    d2 = at(nz, second) + qk - uk * uk / d1
    r1 = 1.0 / jnp.sqrt(d1)
    r2 = 1.0 / jnp.sqrt(d2)
    ratio = uk / d1

    high = aboth.astype(jnp.bfloat16).astype(jnp.float32)
    rest = aboth - high
    mid = rest.astype(jnp.bfloat16).astype(jnp.float32)
    pieces = jnp.where(rid < 2, high, jnp.where(rid < 4, mid, rest - mid)).astype(jnp.bfloat16)
    copy.wait()
    wide = LANES * NB
    for g in range(dense.shape[0]):
        part = slice(wide * g, wide * (g + 1))
        got = matmul(pieces, fvmem[part, :], ((1,), (1,)))
        applied = got[0:2] + got[2:4] + got[4:6]
        left = dense[g][0:2] - applied
        w1 = left[0:1]
        updates[0:1, part] = w1 * r1
        updates[1:2, part] = (left[1:2] - w1 * ratio) * r2


def finish(gmine, gtheirs, pmine, ptheirs, noise, dense, factor, chosen, where):
    local_rows = factor.shape[0]
    vmem = pl.BlockSpec(memory_space=pltpu.VMEM)
    return pl.pallas_call(
        finish_kernel,
        grid_spec=pltpu.PrefetchScalarGridSpec(
            num_scalar_prefetch=2,
            grid=(),
            in_specs=[vmem] * 6 + [pl.BlockSpec(memory_space=pl.ANY)],
            out_specs=[vmem, vmem],
            scratch_shapes=[
                pltpu.VMEM(factor.shape, jnp.bfloat16),
                pltpu.VMEM((R, R), jnp.float32),
                pltpu.VMEM((R, R), jnp.float32),
                pltpu.SemaphoreType.DMA,
            ],
        ),
        out_shape=[
            jax.ShapeDtypeStruct((2, 4), jnp.float32),
            jax.ShapeDtypeStruct((2, local_rows), jnp.float32),
        ],
        compiler_params=pltpu.CompilerParams(vmem_limit_bytes=40 * 2**20),
        name="finish",
    )(chosen, where, gmine, gtheirs, pmine, ptheirs, noise, dense, factor)


def swap_cores(x):
    return lax.ppermute(x, "rows_3", [(0, 1), (1, 0)])


def per_device(factor, cand_weights, cand_block, noise, chosen):
    core = lax.axis_index("rows_3").astype(jnp.int32)
    chip = lax.axis_index(("rows_0", "rows_1", "rows_2")).astype(jnp.int32)
    mine, theirs, dense = local_products(
        factor, cand_weights, cand_block, chosen, core.reshape(1)
    )
    pair = mine + swap_cores(theirs)
    plane = jnp.sum(lax.all_to_all(pair, YX, 0, 0, tiled=True), axis=0)
    shared = jnp.broadcast_to(plane[None, NZ:], (NZ, 2, 8, LANES))
    line = jnp.concatenate([plane[:NZ, None], shared], axis=1)
    summed = jnp.sum(lax.all_to_all(line, "rows_2", 0, 0, tiled=True), axis=0)
    pmine = summed[0]
    ptheirs = swap_cores(pmine)
    copies = jnp.broadcast_to(summed[None, 1:], (NYX, 2, 8, LANES))
    gmine = lax.all_to_all(copies, YX, 0, 0, tiled=True)
    gtheirs = swap_cores(gmine)
    scores, updates = finish(
        gmine, gtheirs, pmine, ptheirs, noise.reshape(8, LANES), dense, factor, chosen,
        jnp.stack([core, chip]),
    )
    return scores, updates


def solution(mesh):
    torus = Mesh(mesh.devices.reshape(4, 4, 8, 2), ROWS)
    return jax.shard_map(
        per_device,
        mesh=torus,
        in_specs=(P(ROWS, None), P(ROWS, None), P(), P(), P()),
        out_specs=(P(None, ROWS), P(None, ROWS)),
        check_vma=False,
    )
```

```python
import jax
import jax.numpy as jnp
from jax import lax
from jax.experimental import pallas as pl
from jax.experimental.pallas import tpu as pltpu
from jax.sharding import Mesh
from jax.sharding import PartitionSpec as P

NB = 4
R = 256
NCAND = 1024
LANES = 128
NYX = 16
NZ = 8
SLOTS = NZ + 2
STEPS = 4
ROWS = ("rows_0", "rows_1", "rows_2", "rows_3")
YX = ("rows_0", "rows_1")
HIGHEST = lax.Precision.HIGHEST


def iota(shape, dim):
    return lax.broadcasted_iota(jnp.int32, shape, dim)


def in_hbm(x):
    return pltpu.with_memory_space_constraint(x, pltpu.HBM)


def matmul(a, b, dims=((1,), (0,)), precision=None):
    return lax.dot_general(
        a, b, (dims, ((), ())), preferred_element_type=jnp.float32, precision=precision
    )


def local_kernel(
    chosen, blocks, core, fac, wts, block_row, mine, theirs, dense,
    fwide, acc, gram, sq8, cross8, masks, wsel, pay,
):
    step = pl.program_id(0)
    wrows = wts.shape[0]
    first, second = chosen[0], chosen[1]

    @pl.when(step == 0)
    def _():
        acc[...] = jnp.zeros_like(acc)
        gram[...] = jnp.zeros_like(gram)
        sq8[...] = jnp.zeros_like(sq8)
        cross8[...] = jnp.zeros_like(cross8)
        pay[:, :, NZ:, :, :] = jnp.zeros((2, NYX, 2, 8, LANES), jnp.float32)
        column = jnp.broadcast_to(block_row[...].astype(jnp.float32), (LANES, NCAND)).T
        for b in range(NB):
            masks[b] = jnp.where(column == float(b), 1.0, 0.0).astype(jnp.bfloat16)

    w = wts[...]
    for h in range(2):
        fwide[h] = fac[:, LANES * h : LANES * (h + 1)].astype(jnp.float32)
    turned = w.T
    total = acc[...]
    gsum = gram[...]
    for b in range(NB):
        fb = jnp.concatenate(
            [fwide[h, pl.ds(b, wrows, stride=NB), :] for h in range(2)], axis=1
        ).astype(jnp.bfloat16)
        mask = masks[b]
        seen = jnp.concatenate(
            [turned[:, LANES * q : LANES * (q + 1)] * mask for q in range(wrows // LANES)], axis=1
        )
        total = total + matmul(seen, fb)
        gsum = gsum + matmul(fb, fb, ((0,), (0,)))
    acc[...] = total
    gram[...] = gsum
    wf = w.astype(jnp.float32)
    sq8[...] += jnp.sum((wf * wf).reshape(wrows // 8, 8, NCAND), axis=0)
    rows = iota((16, LANES), 0)
    lanes = iota((16, LANES), 1)
    picked = jnp.zeros((16, wrows), jnp.float32)
    for row, cand in ((0, first), (1, second)):
        base = pl.multiple_of((cand // LANES) * LANES, LANES)
        hot = jnp.where((rows == row) & (lanes == cand - base), 1.0, 0.0).astype(jnp.bfloat16)
        picked = picked + matmul(hot, wts[:, pl.ds(base, LANES)], ((1,), (1,)))
    cross8[...] += matmul(picked.astype(jnp.bfloat16), w)[:8]
    for q in range(wrows // LANES):
        wsel[step * (wrows // LANES) + q] = picked[:8, LANES * q : LANES * (q + 1)]

    @pl.when(step == STEPS - 1)
    def _():
        proj = acc[...]
        for h in range(2):
            half = proj[:, LANES * h : LANES * (h + 1)]
            pay[h, :, :NZ, :, :] = half.reshape(NYX, NZ, 8, LANES)
        g = gram[...]
        pay[0, :, NZ, :, :] = g[:LANES, :LANES].reshape(NYX, 8, LANES)
        pay[1, :, NZ, :, :] = g[:LANES, LANES:].reshape(NYX, 8, LANES)
        low = g[LANES:, LANES:].reshape(2, NYX // 2, 8, LANES)
        pay[0, : NYX // 2, NZ + 1, :, :] = low[0]
        pay[1, : NYX // 2, NZ + 1, :, :] = low[1]
        for row, cand in ((0, first), (1, second)):
            line = acc[pl.ds(cand, 1), :]
            for h in range(2):
                pay[0, NYX // 2, NZ + 1, 2 * row + h : 2 * row + h + 1, :] = line[
                    :, LANES * h : LANES * (h + 1)
                ]
        sq = jnp.sum(sq8[...], axis=0, keepdims=True)
        same = block_row[...] == blocks[first]
        cross = jnp.where(same, cross8[0:1, :], 0.0)
        for q in range(NCAND // LANES):
            part = slice(LANES * q, LANES * (q + 1))
            pay[1, NYX // 2, NZ + 1, q : q + 1, :] = sq[:, part]
            pay[1, NYX // 2 + 1, NZ + 1, q : q + 1, :] = cross[:, part]
        mine[...] = pay[core[0]]
        theirs[...] = pay[1 - core[0]]
        wide = LANES * NB
        spread = jnp.where(
            iota((LANES, wide), 0) == iota((LANES, wide), 1) // NB, 1.0, 0.0
        ).astype(jnp.bfloat16)
        groups = wsel.shape[0]
        lines = wsel[...].reshape(groups * 8, LANES).astype(jnp.bfloat16)
        repeated = matmul(lines, spread).reshape(groups, 8, wide)
        row = iota((groups, 8, wide), 1)
        place = iota((groups, 8, wide), 2) % NB
        wanted = jnp.where(row == 0, blocks[first], blocks[second])
        dense[...] = jnp.where(place == wanted, repeated, 0.0)


def local_products(factor, cand_weights, cand_block, chosen, core):
    rows, rank = factor.shape
    wrows = cand_weights.shape[0]
    fstep, wstep = rows // STEPS, wrows // STEPS
    groups = wrows // LANES
    payload = jax.ShapeDtypeStruct((NYX, SLOTS, 8, LANES), jnp.float32)
    return pl.pallas_call(
        local_kernel,
        grid_spec=pltpu.PrefetchScalarGridSpec(
            num_scalar_prefetch=3,
            grid=(STEPS,),
            in_specs=[
                pl.BlockSpec((fstep, rank), lambda i, *_: (i, 0)),
                pl.BlockSpec((wstep, NCAND), lambda i, *_: (i, 0)),
                pl.BlockSpec((1, NCAND), lambda i, *_: (0, 0)),
            ],
            out_specs=[pl.BlockSpec(memory_space=pltpu.VMEM)] * 3,
            scratch_shapes=[
                pltpu.VMEM((2, fstep, LANES), jnp.float32),
                pltpu.VMEM((NCAND, rank), jnp.float32),
                pltpu.VMEM((rank, rank), jnp.float32),
                pltpu.VMEM((8, NCAND), jnp.float32),
                pltpu.VMEM((8, NCAND), jnp.float32),
                pltpu.VMEM((NB, NCAND, LANES), jnp.bfloat16),
                pltpu.VMEM((groups, 8, LANES), jnp.float32),
                pltpu.VMEM((2, NYX, SLOTS, 8, LANES), jnp.float32),
            ],
        ),
        out_shape=[payload, payload, jax.ShapeDtypeStruct((groups, 8, LANES * NB), jnp.float32)],
        compiler_params=pltpu.CompilerParams(
            dimension_semantics=("arbitrary",), vmem_limit_bytes=44 * 2**20
        ),
        name="local",
    )(
        chosen,
        cand_block,
        core,
        in_hbm(factor),
        in_hbm(cand_weights),
        cand_block.reshape(1, NCAND),
    )


def total(x):
    return jnp.sum(jnp.sum(x, axis=1, keepdims=True), axis=0, keepdims=True)


def lane_sum(x):
    return jnp.sum(x, axis=1, keepdims=True)


def finish_kernel(
    chosen, where, gmine, gtheirs, pmine, ptheirs, noise, dense, factor, scores, updates,
    fvmem, m, x, sem,
):
    copy = pltpu.make_async_copy(factor, fvmem, sem)
    copy.start()
    core, chip = where[0], where[1]
    first, second = chosen[0], chosen[1]
    own = core == 0
    a_, b_ = gmine[...], gtheirs[...]
    g0 = jnp.where(own, a_, b_)
    g1 = jnp.where(own, b_, a_)
    half = NYX // 2
    top = g0[:, 0].reshape(LANES, LANES)
    side = g1[:, 0].reshape(LANES, LANES)
    low = jnp.concatenate([g0[:half, 1], g1[:half, 1]], axis=0).reshape(LANES, LANES)
    diag = iota((LANES, LANES), 0) == iota((LANES, LANES), 1)
    m[:LANES, :LANES] = top + jnp.where(diag, 1.0, 0.0)
    m[:LANES, LANES:] = side
    m[LANES:, :LANES] = side.T
    m[LANES:, LANES:] = low + jnp.where(diag, 1.0, 0.0)
    psel, sq, cross = g0[half, 1], g1[half, 1], g1[half + 1, 1]
    p_, q_ = pmine[...], ptheirs[...]
    pown = jnp.concatenate([jnp.where(own, p_, q_), jnp.where(own, q_, p_)], axis=1)
    pj = jnp.concatenate([psel[0:1], psel[1:2]], axis=1)
    pk = jnp.concatenate([psel[2:3], psel[3:4]], axis=1)
    rid = iota((8, R), 0)
    pboth = jnp.where(rid >= 6, 0.0, jnp.where(rid % 2 == 0, pj, pk))
    rhs = jnp.concatenate([pown, pboth], axis=0)

    full = m[...]
    rowmax = jnp.max(jnp.sum(jnp.abs(full), axis=0, keepdims=True))
    bound = jnp.maximum(rowmax, 1.0)
    rho0 = (bound - 1.0) / (bound + 1.0)
    alpha = 2.0 / (bound + 1.0)
    eye = jnp.where(iota((R, R), 0) == iota((R, R), 1), 1.0, 0.0)
    scale0 = 2.0 / (2.0 - rho0 * rho0)
    x[...] = (scale0 * alpha) * (2.0 * eye - alpha * full)
    rho1 = rho0 * rho0 / (2.0 - rho0 * rho0)

    def newton(carry):
        rho, count = carry
        scale = 2.0 / (2.0 - rho * rho)
        now = x[...]
        prod = matmul(m[...], now, precision=HIGHEST)
        x[...] = scale * (2.0 * now - matmul(now, prod, precision=HIGHEST))
        return rho * rho / (2.0 - rho * rho), count + 1

    lax.while_loop(lambda s: (s[0] > 5e-3) & (s[1] < 100), newton, (rho1, jnp.int32(0)))
    inv = x[...]
    a = matmul(rhs, inv, precision=HIGHEST)
    for _ in range(2):
        left = rhs - matmul(a, full, precision=HIGHEST)
        a = a + matmul(left, inv, precision=HIGHEST)

    aown, aboth = a[:8], a[8:]
    aj, ak = aboth[0:1], aboth[1:2]
    rows = iota((8, LANES), 0)
    lanes = iota((8, LANES), 1)
    flat = rows * LANES + lanes
    nz = noise[...]

    def at(tile, cand):
        return total(jnp.where(flat == cand, tile, 0.0))

    def owned(tile):
        line = jnp.sum(jnp.where(rows == chip // NYX, tile, 0.0), axis=0, keepdims=True)
        return lane_sum(jnp.where(lanes == (chip % NYX) * 8 + rows, line, 0.0))

    sqc, crossc, noisec = owned(sq), owned(cross), owned(nz)
    pa = lane_sum(pown * aown)
    aa = lane_sum(aown * aown)
    pja = lane_sum(aown * pj)
    aja = lane_sum(aown * aj)
    q = sqc - pa
    nrm = sqc - 2.0 * pa + (pa - aa)
    paj = lane_sum(pj * aj)
    qj = at(sq, first) - paj
    big = at(sq, first) - 2.0 * paj + (paj - lane_sum(aj * aj))
    d1 = at(nz, first) + qj
    u = crossc - pja
    e = u - aja
    q2 = q - u * u / d1
    nrm2 = nrm - 2.0 * u * e / d1 + u * u * big / (d1 * d1)
    for row, s in ((0, nrm / (noisec + q)), (1, nrm2 / (noisec + q2))):
        line = jnp.sum(jnp.where(rows == lanes + 4 * core, s, 0.0), axis=0, keepdims=True)
        scores[row : row + 1, :] = line[:, :4]
    uk = at(cross, second) - lane_sum(pj * ak)
    qk = at(sq, second) - lane_sum(pk * ak)
    d2 = at(nz, second) + qk - uk * uk / d1
    r1 = 1.0 / jnp.sqrt(d1)
    r2 = 1.0 / jnp.sqrt(d2)
    ratio = uk / d1

    high = aboth.astype(jnp.bfloat16).astype(jnp.float32)
    rest = aboth - high
    mid = rest.astype(jnp.bfloat16).astype(jnp.float32)
    pieces = jnp.where(rid < 2, high, jnp.where(rid < 4, mid, rest - mid)).astype(jnp.bfloat16)
    copy.wait()
    wide = LANES * NB
    for g in range(dense.shape[0]):
        part = slice(wide * g, wide * (g + 1))
        got = matmul(pieces, fvmem[part, :], ((1,), (1,)))
        applied = got[0:2] + got[2:4] + got[4:6]
        left = dense[g][0:2] - applied
        w1 = left[0:1]
        updates[0:1, part] = w1 * r1
        updates[1:2, part] = (left[1:2] - w1 * ratio) * r2


def finish(gmine, gtheirs, pmine, ptheirs, noise, dense, factor, chosen, where):
    local_rows = factor.shape[0]
    vmem = pl.BlockSpec(memory_space=pltpu.VMEM)
    return pl.pallas_call(
        finish_kernel,
        grid_spec=pltpu.PrefetchScalarGridSpec(
            num_scalar_prefetch=2,
            grid=(),
            in_specs=[vmem] * 6 + [pl.BlockSpec(memory_space=pl.ANY)],
            out_specs=[vmem, vmem],
            scratch_shapes=[
                pltpu.VMEM(factor.shape, jnp.bfloat16),
                pltpu.VMEM((R, R), jnp.float32),
                pltpu.VMEM((R, R), jnp.float32),
                pltpu.SemaphoreType.DMA,
            ],
        ),
        out_shape=[
            jax.ShapeDtypeStruct((2, 4), jnp.float32),
            jax.ShapeDtypeStruct((2, local_rows), jnp.float32),
        ],
        compiler_params=pltpu.CompilerParams(vmem_limit_bytes=16 * 2**20),
        name="finish",
    )(chosen, where, gmine, gtheirs, pmine, ptheirs, noise, dense, in_hbm(factor))


def swap_cores(x):
    return lax.ppermute(x, "rows_3", [(0, 1), (1, 0)])


def per_device(factor, cand_weights, cand_block, noise, chosen):
    core = lax.axis_index("rows_3").astype(jnp.int32)
    chip = lax.axis_index(("rows_0", "rows_1", "rows_2")).astype(jnp.int32)
    mine, theirs, dense = local_products(
        factor, cand_weights, cand_block, chosen, core.reshape(1)
    )
    pair = mine + swap_cores(theirs)
    plane = jnp.sum(lax.all_to_all(pair, YX, 0, 0, tiled=True), axis=0)
    shared = jnp.broadcast_to(plane[None, NZ:], (NZ, 2, 8, LANES))
    line = jnp.concatenate([plane[:NZ, None], shared], axis=1)
    summed = jnp.sum(lax.all_to_all(line, "rows_2", 0, 0, tiled=True), axis=0)
    pmine = summed[0]
    ptheirs = swap_cores(pmine)
    copies = jnp.broadcast_to(summed[None, 1:], (NYX, 2, 8, LANES))
    gmine = lax.all_to_all(copies, YX, 0, 0, tiled=True)
    gtheirs = swap_cores(gmine)
    scores, updates = finish(
        gmine, gtheirs, pmine, ptheirs, noise.reshape(8, LANES), dense, factor, chosen,
        jnp.stack([core, chip]),
    )
    return scores, updates


def solution(mesh):
    torus = Mesh(mesh.devices.reshape(4, 4, 8, 2), ROWS)
    return jax.shard_map(
        per_device,
        mesh=torus,
        in_specs=(P(ROWS, None), P(ROWS, None), P(), P(), P()),
        out_specs=(P(None, ROWS), P(None, ROWS)),
        check_vma=False,
    )
```

```python
import jax
import jax.numpy as jnp
from jax import lax
from jax.experimental import pallas as pl
from jax.experimental.pallas import tpu as pltpu
from jax.sharding import Mesh
from jax.sharding import PartitionSpec as P

NB = 4
R = 256
NCAND = 1024
LANES = 128
NYX = 16
NZ = 8
SLOTS = NZ + 2
STEPS = 4
MILD = 1024.0
ROWS = ("rows_0", "rows_1", "rows_2", "rows_3")
YX = ("rows_0", "rows_1")
HIGHEST = lax.Precision.HIGHEST


def iota(shape, dim):
    return lax.broadcasted_iota(jnp.int32, shape, dim)


def in_hbm(x):
    return pltpu.with_memory_space_constraint(x, pltpu.HBM)


def matmul(a, b, dims=((1,), (0,)), precision=None):
    return lax.dot_general(
        a, b, (dims, ((), ())), preferred_element_type=jnp.float32, precision=precision
    )


def local_kernel(
    chosen, blocks, core, fac, wts, block_row, mine, theirs, dense,
    fwide, acc, gram, sq8, cross8, masks, wsel, pay,
):
    step = pl.program_id(0)
    wrows = wts.shape[0]
    first, second = chosen[0], chosen[1]

    @pl.when(step == 0)
    def _():
        acc[...] = jnp.zeros_like(acc)
        gram[...] = jnp.zeros_like(gram)
        sq8[...] = jnp.zeros_like(sq8)
        cross8[...] = jnp.zeros_like(cross8)
        pay[:, :, NZ:, :, :] = jnp.zeros((2, NYX, 2, 8, LANES), jnp.float32)
        column = jnp.broadcast_to(block_row[...].astype(jnp.float32), (LANES, NCAND)).T
        for b in range(NB):
            masks[b] = jnp.where(column == float(b), 1.0, 0.0).astype(jnp.bfloat16)

    w = wts[...]
    for h in range(2):
        fwide[h] = fac[:, LANES * h : LANES * (h + 1)].astype(jnp.float32)
    turned = w.T
    total = acc[...]
    gsum = gram[...]
    for b in range(NB):
        fb = jnp.concatenate(
            [fwide[h, pl.ds(b, wrows, stride=NB), :] for h in range(2)], axis=1
        ).astype(jnp.bfloat16)
        mask = masks[b]
        seen = jnp.concatenate(
            [turned[:, LANES * q : LANES * (q + 1)] * mask for q in range(wrows // LANES)], axis=1
        )
        total = total + matmul(seen, fb)
        gsum = gsum + matmul(fb, fb, ((0,), (0,)))
    acc[...] = total
    gram[...] = gsum
    wf = w.astype(jnp.float32)
    sq8[...] += jnp.sum((wf * wf).reshape(wrows // 8, 8, NCAND), axis=0)
    rows = iota((16, LANES), 0)
    lanes = iota((16, LANES), 1)
    picked = jnp.zeros((16, wrows), jnp.float32)
    for row, cand in ((0, first), (1, second)):
        base = pl.multiple_of((cand // LANES) * LANES, LANES)
        hot = jnp.where((rows == row) & (lanes == cand - base), 1.0, 0.0).astype(jnp.bfloat16)
        picked = picked + matmul(hot, wts[:, pl.ds(base, LANES)], ((1,), (1,)))
    cross8[...] += matmul(picked.astype(jnp.bfloat16), w)[:8]
    for q in range(wrows // LANES):
        wsel[step * (wrows // LANES) + q] = picked[:8, LANES * q : LANES * (q + 1)]

    @pl.when(step == STEPS - 1)
    def _():
        proj = acc[...]
        for h in range(2):
            half = proj[:, LANES * h : LANES * (h + 1)]
            pay[h, :, :NZ, :, :] = half.reshape(NYX, NZ, 8, LANES)
        g = gram[...]
        pay[0, :, NZ, :, :] = g[:LANES, :LANES].reshape(NYX, 8, LANES)
        pay[1, :, NZ, :, :] = g[:LANES, LANES:].reshape(NYX, 8, LANES)
        low = g[LANES:, LANES:].reshape(2, NYX // 2, 8, LANES)
        pay[0, : NYX // 2, NZ + 1, :, :] = low[0]
        pay[1, : NYX // 2, NZ + 1, :, :] = low[1]
        for row, cand in ((0, first), (1, second)):
            line = acc[pl.ds(cand, 1), :]
            for h in range(2):
                pay[0, NYX // 2, NZ + 1, 2 * row + h : 2 * row + h + 1, :] = line[
                    :, LANES * h : LANES * (h + 1)
                ]
        sq = jnp.sum(sq8[...], axis=0, keepdims=True)
        same = block_row[...] == blocks[first]
        cross = jnp.where(same, cross8[0:1, :], 0.0)
        for q in range(NCAND // LANES):
            part = slice(LANES * q, LANES * (q + 1))
            pay[1, NYX // 2, NZ + 1, q : q + 1, :] = sq[:, part]
            pay[1, NYX // 2 + 1, NZ + 1, q : q + 1, :] = cross[:, part]
        mine[...] = pay[core[0]]
        theirs[...] = pay[1 - core[0]]
        wide = LANES * NB
        spread = jnp.where(
            iota((LANES, wide), 0) == iota((LANES, wide), 1) // NB, 1.0, 0.0
        ).astype(jnp.bfloat16)
        groups = wsel.shape[0]
        lines = wsel[...].reshape(groups * 8, LANES).astype(jnp.bfloat16)
        repeated = matmul(lines, spread).reshape(groups, 8, wide)
        row = iota((groups, 8, wide), 1)
        place = iota((groups, 8, wide), 2) % NB
        wanted = jnp.where(row == 0, blocks[first], blocks[second])
        dense[...] = jnp.where(place == wanted, repeated, 0.0)


def local_products(factor, cand_weights, cand_block, chosen, core):
    rows, rank = factor.shape
    wrows = cand_weights.shape[0]
    fstep, wstep = rows // STEPS, wrows // STEPS
    groups = wrows // LANES
    payload = jax.ShapeDtypeStruct((NYX, SLOTS, 8, LANES), jnp.float32)
    return pl.pallas_call(
        local_kernel,
        grid_spec=pltpu.PrefetchScalarGridSpec(
            num_scalar_prefetch=3,
            grid=(STEPS,),
            in_specs=[
                pl.BlockSpec((fstep, rank), lambda i, *_: (i, 0)),
                pl.BlockSpec((wstep, NCAND), lambda i, *_: (i, 0)),
                pl.BlockSpec((1, NCAND), lambda i, *_: (0, 0)),
            ],
            out_specs=[pl.BlockSpec(memory_space=pltpu.VMEM)] * 3,
            scratch_shapes=[
                pltpu.VMEM((2, fstep, LANES), jnp.float32),
                pltpu.VMEM((NCAND, rank), jnp.float32),
                pltpu.VMEM((rank, rank), jnp.float32),
                pltpu.VMEM((8, NCAND), jnp.float32),
                pltpu.VMEM((8, NCAND), jnp.float32),
                pltpu.VMEM((NB, NCAND, LANES), jnp.bfloat16),
                pltpu.VMEM((groups, 8, LANES), jnp.float32),
                pltpu.VMEM((2, NYX, SLOTS, 8, LANES), jnp.float32),
            ],
        ),
        out_shape=[payload, payload, jax.ShapeDtypeStruct((groups, 8, LANES * NB), jnp.float32)],
        compiler_params=pltpu.CompilerParams(
            dimension_semantics=("arbitrary",), vmem_limit_bytes=44 * 2**20
        ),
        name="local",
    )(
        in_hbm(chosen),
        in_hbm(cand_block),
        core,
        in_hbm(factor),
        in_hbm(cand_weights),
        cand_block.reshape(1, NCAND),
    )


def parts(x):
    high = x.astype(jnp.bfloat16)
    return high, (x - high.astype(jnp.float32)).astype(jnp.bfloat16)


def paired(p, q):
    ph, pl_ = parts(p)
    qh, ql = parts(q)
    return matmul(
        jnp.concatenate([ph, pl_, ph], axis=1), jnp.concatenate([qh, qh, ql], axis=0)
    )


def total(x):
    return jnp.sum(jnp.sum(x, axis=1, keepdims=True), axis=0, keepdims=True)


def lane_sum(x):
    return jnp.sum(x, axis=1, keepdims=True)


def finish_kernel(
    chosen, where, mine, theirs, noise, dense, factor, scores, updates,
    fvmem, m, x, sem,
):
    copy = pltpu.make_async_copy(factor, fvmem, sem)
    copy.start()
    core, chip = where[0], where[1]
    first, second = chosen[0], chosen[1]
    own = core == 0
    a_, b_ = mine[...], theirs[...]
    first_half = jnp.where(own, a_, b_)
    second_half = jnp.where(own, b_, a_)
    g0 = first_half[: 2 * NYX].reshape(NYX, 2, 8, LANES)
    g1 = second_half[: 2 * NYX].reshape(NYX, 2, 8, LANES)
    half = NYX // 2
    top = g0[:, 0].reshape(LANES, LANES)
    side = g1[:, 0].reshape(LANES, LANES)
    low = jnp.concatenate([g0[:half, 1], g1[:half, 1]], axis=0).reshape(LANES, LANES)
    diag = iota((LANES, LANES), 0) == iota((LANES, LANES), 1)
    m[:LANES, :LANES] = top + jnp.where(diag, 1.0, 0.0)
    m[:LANES, LANES:] = side
    m[LANES:, :LANES] = side.T
    m[LANES:, LANES:] = low + jnp.where(diag, 1.0, 0.0)
    psel, sq, cross = g0[half, 1], g1[half, 1], g1[half + 1, 1]
    pown = jnp.concatenate([first_half[2 * NYX], second_half[2 * NYX]], axis=1)
    pj = jnp.concatenate([psel[0:1], psel[1:2]], axis=1)
    pk = jnp.concatenate([psel[2:3], psel[3:4]], axis=1)
    rid = iota((8, R), 0)
    pboth = jnp.where(rid >= 6, 0.0, jnp.where(rid % 2 == 0, pj, pk))
    rhs = jnp.concatenate([pown, pboth], axis=0)

    full = m[...]
    rowmax = jnp.max(jnp.sum(jnp.abs(full), axis=0, keepdims=True))
    bound = jnp.maximum(rowmax, 1.0)
    rho0 = (bound - 1.0) / (bound + 1.0)
    alpha = 2.0 / (bound + 1.0)
    eye = jnp.where(iota((R, R), 0) == iota((R, R), 1), 1.0, 0.0)
    scale0 = 2.0 / (2.0 - rho0 * rho0)
    x[...] = (scale0 * alpha) * (2.0 * eye - alpha * full)
    rho1 = rho0 * rho0 / (2.0 - rho0 * rho0)

    def precise(p, q):
        return matmul(p, q, precision=HIGHEST)

    def newton(product):
        def body(carry):
            rho, count = carry
            scale = 2.0 / (2.0 - rho * rho)
            now = x[...]
            x[...] = scale * (2.0 * now - product(now, product(m[...], now)))
            return rho * rho / (2.0 - rho * rho), count + 1

        return body

    mild = bound < MILD
    state = lax.while_loop(
        lambda s: mild & (s[0] > 5e-3) & (s[1] < 100), newton(paired), (rho1, jnp.int32(0))
    )
    lax.while_loop(lambda s: (s[0] > 5e-3) & (s[1] < 100), newton(precise), state)

    def solved(product):
        inv, system = x[...], m[...]
        a = product(rhs, inv)
        for _ in range(2):
            a = a + product(rhs - precise(a, system), inv)
        return a

    a = lax.cond(mild, lambda: solved(paired), lambda: solved(precise))

    aown, aboth = a[:8], a[8:]
    aj, ak = aboth[0:1], aboth[1:2]
    rows = iota((8, LANES), 0)
    lanes = iota((8, LANES), 1)
    flat = rows * LANES + lanes
    nz = noise[...]

    def at(tile, cand):
        return total(jnp.where(flat == cand, tile, 0.0))

    def owned(tile):
        line = jnp.sum(jnp.where(rows == chip // NYX, tile, 0.0), axis=0, keepdims=True)
        return lane_sum(jnp.where(lanes == (chip % NYX) * 8 + rows, line, 0.0))

    sqc, crossc, noisec = owned(sq), owned(cross), owned(nz)
    pa = lane_sum(pown * aown)
    aa = lane_sum(aown * aown)
    pja = lane_sum(aown * pj)
    aja = lane_sum(aown * aj)
    q = sqc - pa
    nrm = sqc - 2.0 * pa + (pa - aa)
    paj = lane_sum(pj * aj)
    qj = at(sq, first) - paj
    big = at(sq, first) - 2.0 * paj + (paj - lane_sum(aj * aj))
    d1 = at(nz, first) + qj
    u = crossc - pja
    e = u - aja
    q2 = q - u * u / d1
    nrm2 = nrm - 2.0 * u * e / d1 + u * u * big / (d1 * d1)
    for row, s in ((0, nrm / (noisec + q)), (1, nrm2 / (noisec + q2))):
        line = jnp.sum(jnp.where(rows == lanes + 4 * core, s, 0.0), axis=0, keepdims=True)
        scores[row : row + 1, :] = line[:, :4]
    uk = at(cross, second) - lane_sum(pj * ak)
    qk = at(sq, second) - lane_sum(pk * ak)
    d2 = at(nz, second) + qk - uk * uk / d1
    r1 = 1.0 / jnp.sqrt(d1)
    r2 = 1.0 / jnp.sqrt(d2)
    ratio = uk / d1

    high = aboth.astype(jnp.bfloat16).astype(jnp.float32)
    rest = aboth - high
    mid = rest.astype(jnp.bfloat16).astype(jnp.float32)
    pieces = jnp.where(rid < 2, high, jnp.where(rid < 4, mid, rest - mid)).astype(jnp.bfloat16)
    copy.wait()
    wide = LANES * NB
    for g in range(dense.shape[0]):
        part = slice(wide * g, wide * (g + 1))
        got = matmul(pieces, fvmem[part, :], ((1,), (1,)))
        applied = got[0:2] + got[2:4] + got[4:6]
        left = dense[g][0:2] - applied
        w1 = left[0:1]
        updates[0:1, part] = w1 * r1
        updates[1:2, part] = (left[1:2] - w1 * ratio) * r2


def finish(mine, theirs, noise, dense, factor, chosen, where):
    local_rows = factor.shape[0]
    vmem = pl.BlockSpec(memory_space=pltpu.VMEM)
    return pl.pallas_call(
        finish_kernel,
        grid_spec=pltpu.PrefetchScalarGridSpec(
            num_scalar_prefetch=2,
            grid=(),
            in_specs=[vmem] * 4 + [pl.BlockSpec(memory_space=pl.ANY)],
            out_specs=[vmem, vmem],
            scratch_shapes=[
                pltpu.VMEM(factor.shape, jnp.bfloat16),
                pltpu.VMEM((R, R), jnp.float32),
                pltpu.VMEM((R, R), jnp.float32),
                pltpu.SemaphoreType.DMA,
            ],
        ),
        out_shape=[
            jax.ShapeDtypeStruct((2, 4), jnp.float32),
            jax.ShapeDtypeStruct((2, local_rows), jnp.float32),
        ],
        compiler_params=pltpu.CompilerParams(vmem_limit_bytes=16 * 2**20),
        name="finish",
    )(in_hbm(chosen), where, mine, theirs, noise, dense, in_hbm(factor))


def swap_cores(x):
    return lax.ppermute(x, "rows_3", [(0, 1), (1, 0)])


def per_device(factor, cand_weights, cand_block, noise, chosen):
    core = lax.axis_index("rows_3").astype(jnp.int32)
    chip = lax.axis_index(("rows_0", "rows_1", "rows_2")).astype(jnp.int32)
    where = jnp.stack([core, chip])
    mine, theirs, dense = local_products(factor, cand_weights, cand_block, chosen, where)
    pair = mine + swap_cores(theirs)
    plane = jnp.sum(lax.all_to_all(pair, YX, 0, 0, tiled=True), axis=0)
    shared = jnp.broadcast_to(plane[None, NZ:], (NZ, 2, 8, LANES))
    line = jnp.concatenate([plane[:NZ, None], shared], axis=1)
    summed = jnp.sum(lax.all_to_all(line, "rows_2", 0, 0, tiled=True), axis=0)
    shared = jnp.broadcast_to(summed[None, 1:], (NYX, 2, 8, LANES))
    shared, own = lax.optimization_barrier((shared, summed[:1]))
    gathered = lax.all_to_all(shared, YX, 0, 0, tiled=True)
    known = jnp.concatenate([gathered.reshape(2 * NYX, 8, LANES), own], axis=0)
    scores, updates = finish(
        known, swap_cores(known), noise.reshape(8, LANES), dense, factor, chosen, where
    )
    return scores, updates


def solution(mesh):
    torus = Mesh(mesh.devices.reshape(4, 4, 8, 2), ROWS)
    return jax.shard_map(
        per_device,
        mesh=torus,
        in_specs=(P(ROWS, None), P(ROWS, None), P(), P(), P()),
        out_specs=(P(None, ROWS), P(None, ROWS)),
        check_vma=False,
    )
```

```python
import jax
import jax.numpy as jnp
from jax import lax
from jax.experimental import pallas as pl
from jax.experimental.pallas import tpu as pltpu
from jax.sharding import Mesh
from jax.sharding import PartitionSpec as P

NB = 4
R = 256
NCAND = 1024
LANES = 128
NYX = 16
NZ = 8
SLOTS = NZ + 2
STEPS = 4
MILD = 1024.0
RHO = 1e-2
ROWS = ("rows_0", "rows_1", "rows_2", "rows_3")
YX = ("rows_0", "rows_1")
HIGHEST = lax.Precision.HIGHEST


def iota(shape, dim):
    return lax.broadcasted_iota(jnp.int32, shape, dim)


def in_hbm(x):
    return pltpu.with_memory_space_constraint(x, pltpu.HBM)


def matmul(a, b, dims=((1,), (0,)), precision=None):
    return lax.dot_general(
        a, b, (dims, ((), ())), preferred_element_type=jnp.float32, precision=precision
    )


def local_kernel(
    chosen, blocks, core, fac, wts, block_row, mine, theirs, dense,
    fwide, acc, gram, sq8, cross8, masks, wsel, pay,
):
    step = pl.program_id(0)
    wrows = wts.shape[0]
    first, second = chosen[0], chosen[1]

    @pl.when(step == 0)
    def _():
        acc[...] = jnp.zeros_like(acc)
        gram[...] = jnp.zeros_like(gram)
        sq8[...] = jnp.zeros_like(sq8)
        cross8[...] = jnp.zeros_like(cross8)
        pay[:, :, NZ:, :, :] = jnp.zeros((2, NYX, 2, 8, LANES), jnp.float32)
        column = jnp.broadcast_to(block_row[...].astype(jnp.float32), (LANES, NCAND)).T
        for b in range(NB):
            masks[b] = jnp.where(column == float(b), 1.0, 0.0).astype(jnp.bfloat16)

    w = wts[...]
    for h in range(2):
        fwide[h] = fac[:, LANES * h : LANES * (h + 1)].astype(jnp.float32)
    turned = w.T
    total = acc[...]
    gsum = gram[...]
    for b in range(NB):
        fb = jnp.concatenate(
            [fwide[h, pl.ds(b, wrows, stride=NB), :] for h in range(2)], axis=1
        ).astype(jnp.bfloat16)
        mask = masks[b]
        seen = jnp.concatenate(
            [turned[:, LANES * q : LANES * (q + 1)] * mask for q in range(wrows // LANES)], axis=1
        )
        total = total + matmul(seen, fb)
        gsum = gsum + matmul(fb, fb, ((0,), (0,)))
    acc[...] = total
    gram[...] = gsum
    wf = w.astype(jnp.float32)
    sq8[...] += jnp.sum((wf * wf).reshape(wrows // 8, 8, NCAND), axis=0)
    rows = iota((16, LANES), 0)
    lanes = iota((16, LANES), 1)
    picked = jnp.zeros((16, wrows), jnp.float32)
    for row, cand in ((0, first), (1, second)):
        base = pl.multiple_of((cand // LANES) * LANES, LANES)
        hot = jnp.where((rows == row) & (lanes == cand - base), 1.0, 0.0).astype(jnp.bfloat16)
        picked = picked + matmul(hot, wts[:, pl.ds(base, LANES)], ((1,), (1,)))
    cross8[...] += matmul(picked.astype(jnp.bfloat16), w)[:8]
    for q in range(wrows // LANES):
        wsel[step * (wrows // LANES) + q] = picked[:8, LANES * q : LANES * (q + 1)]

    @pl.when(step == STEPS - 1)
    def _():
        proj = acc[...]
        for h in range(2):
            half = proj[:, LANES * h : LANES * (h + 1)]
            pay[h, :, :NZ, :, :] = half.reshape(NYX, NZ, 8, LANES)
        g = gram[...]
        pay[0, :, NZ, :, :] = g[:LANES, :LANES].reshape(NYX, 8, LANES)
        pay[1, :, NZ, :, :] = g[:LANES, LANES:].reshape(NYX, 8, LANES)
        low = g[LANES:, LANES:].reshape(2, NYX // 2, 8, LANES)
        pay[0, : NYX // 2, NZ + 1, :, :] = low[0]
        pay[1, : NYX // 2, NZ + 1, :, :] = low[1]
        for row, cand in ((0, first), (1, second)):
            line = acc[pl.ds(cand, 1), :]
            for h in range(2):
                pay[0, NYX // 2, NZ + 1, 2 * row + h : 2 * row + h + 1, :] = line[
                    :, LANES * h : LANES * (h + 1)
                ]
        sq = jnp.sum(sq8[...], axis=0, keepdims=True)
        same = block_row[...] == blocks[first]
        cross = jnp.where(same, cross8[0:1, :], 0.0)
        for q in range(NCAND // LANES):
            part = slice(LANES * q, LANES * (q + 1))
            pay[1, NYX // 2, NZ + 1, q : q + 1, :] = sq[:, part]
            pay[1, NYX // 2 + 1, NZ + 1, q : q + 1, :] = cross[:, part]
        mine[...] = pay[core[0]]
        theirs[...] = pay[1 - core[0]]
        wide = LANES * NB
        spread = jnp.where(
            iota((LANES, wide), 0) == iota((LANES, wide), 1) // NB, 1.0, 0.0
        ).astype(jnp.bfloat16)
        groups = wsel.shape[0]
        lines = wsel[...].reshape(groups * 8, LANES).astype(jnp.bfloat16)
        repeated = matmul(lines, spread).reshape(groups, 8, wide)
        row = iota((groups, 8, wide), 1)
        place = iota((groups, 8, wide), 2) % NB
        wanted = jnp.where(row == 0, blocks[first], blocks[second])
        dense[...] = jnp.where(place == wanted, repeated, 0.0)


def local_products(factor, cand_weights, cand_block, chosen, core):
    rows, rank = factor.shape
    wrows = cand_weights.shape[0]
    fstep, wstep = rows // STEPS, wrows // STEPS
    groups = wrows // LANES
    payload = jax.ShapeDtypeStruct((NYX, SLOTS, 8, LANES), jnp.float32)
    return pl.pallas_call(
        local_kernel,
        grid_spec=pltpu.PrefetchScalarGridSpec(
            num_scalar_prefetch=3,
            grid=(STEPS,),
            in_specs=[
                pl.BlockSpec((fstep, rank), lambda i, *_: (i, 0)),
                pl.BlockSpec((wstep, NCAND), lambda i, *_: (i, 0)),
                pl.BlockSpec((1, NCAND), lambda i, *_: (0, 0)),
            ],
            out_specs=[pl.BlockSpec(memory_space=pltpu.VMEM)] * 3,
            scratch_shapes=[
                pltpu.VMEM((2, fstep, LANES), jnp.float32),
                pltpu.VMEM((NCAND, rank), jnp.float32),
                pltpu.VMEM((rank, rank), jnp.float32),
                pltpu.VMEM((8, NCAND), jnp.float32),
                pltpu.VMEM((8, NCAND), jnp.float32),
                pltpu.VMEM((NB, NCAND, LANES), jnp.bfloat16),
                pltpu.VMEM((groups, 8, LANES), jnp.float32),
                pltpu.VMEM((2, NYX, SLOTS, 8, LANES), jnp.float32),
            ],
        ),
        out_shape=[payload, payload, jax.ShapeDtypeStruct((groups, 8, LANES * NB), jnp.float32)],
        compiler_params=pltpu.CompilerParams(
            dimension_semantics=("arbitrary",), vmem_limit_bytes=44 * 2**20
        ),
        name="local",
    )(
        in_hbm(chosen),
        in_hbm(cand_block),
        core,
        in_hbm(factor),
        in_hbm(cand_weights),
        cand_block.reshape(1, NCAND),
    )


def parts(x):
    high = x.astype(jnp.bfloat16)
    return high, (x - high.astype(jnp.float32)).astype(jnp.bfloat16)


def paired(p, q):
    ph, pl_ = parts(p)
    qh, ql = parts(q)
    return matmul(
        jnp.concatenate([ph, pl_, ph], axis=1), jnp.concatenate([qh, qh, ql], axis=0)
    )


def total(x):
    return jnp.sum(jnp.sum(x, axis=1, keepdims=True), axis=0, keepdims=True)


def lane_sum(x):
    return jnp.sum(x, axis=1, keepdims=True)


def finish_kernel(
    chosen, where, mine, theirs, noise, dense, factor, scores, updates,
    fvmem, m, x, sem,
):
    copy = pltpu.make_async_copy(factor, fvmem, sem)
    copy.start()
    core, chip = where[0], where[1]
    first, second = chosen[0], chosen[1]
    own = core == 0
    a_, b_ = mine[...], theirs[...]
    first_half = jnp.where(own, a_, b_)
    second_half = jnp.where(own, b_, a_)
    g0 = first_half[: 2 * NYX].reshape(NYX, 2, 8, LANES)
    g1 = second_half[: 2 * NYX].reshape(NYX, 2, 8, LANES)
    half = NYX // 2
    top = g0[:, 0].reshape(LANES, LANES)
    side = g1[:, 0].reshape(LANES, LANES)
    low = jnp.concatenate([g0[:half, 1], g1[:half, 1]], axis=0).reshape(LANES, LANES)
    diag = iota((LANES, LANES), 0) == iota((LANES, LANES), 1)
    m[:LANES, :LANES] = top + jnp.where(diag, 1.0, 0.0)
    m[:LANES, LANES:] = side
    m[LANES:, :LANES] = side.T
    m[LANES:, LANES:] = low + jnp.where(diag, 1.0, 0.0)
    psel, sq, cross = g0[half, 1], g1[half, 1], g1[half + 1, 1]
    pown = jnp.concatenate([first_half[2 * NYX], second_half[2 * NYX]], axis=1)
    pj = jnp.concatenate([psel[0:1], psel[1:2]], axis=1)
    pk = jnp.concatenate([psel[2:3], psel[3:4]], axis=1)
    rid = iota((8, R), 0)
    pboth = jnp.where(rid >= 6, 0.0, jnp.where(rid % 2 == 0, pj, pk))
    rhs = jnp.concatenate([pown, pboth], axis=0)

    full = m[...]
    reach = jnp.max(jnp.sum(jnp.abs(full), axis=0, keepdims=True))
    mild = reach < MILD
    unit = full * (1.0 / reach)

    def precise(p, q):
        return matmul(p, q, precision=HIGHEST)

    @pl.when(mild)
    def _():
        x[...] = paired(unit, unit)

    @pl.when(jnp.logical_not(mild))
    def _():
        x[...] = precise(unit, unit)

    square = x[...]
    norm = jnp.sqrt(jnp.max(total(square * square)))
    bound = jnp.maximum(reach * jnp.minimum(1.001 * jnp.sqrt(norm), 1.0), 1.0)
    rho0 = (bound - 1.0) / (bound + 1.0)
    alpha = 2.0 / (bound + 1.0)
    grow = alpha * (2.0 / (2.0 - rho0 * rho0))
    rho1 = rho0 * rho0 / (2.0 - rho0 * rho0)
    scale1 = 2.0 / (2.0 - rho1 * rho1)
    eye = jnp.where(iota((R, R), 0) == iota((R, R), 1), 1.0, 0.0)
    start = grow * (2.0 * eye - alpha * full)
    prod1 = (grow * reach) * (2.0 * unit - (alpha * reach) * square)

    def newton(product):
        def body(carry):
            rho, count = carry
            scale = 2.0 / (2.0 - rho * rho)
            now = x[...]
            x[...] = scale * (2.0 * now - product(now, product(m[...], now)))
            return rho * rho / (2.0 - rho * rho), count + 1

        return body

    @pl.when(mild)
    def _():
        x[...] = scale1 * (2.0 * start - paired(start, prod1))

    @pl.when(jnp.logical_not(mild))
    def _():
        x[...] = scale1 * (2.0 * start - precise(start, prod1))

    rho2 = rho1 * rho1 / (2.0 - rho1 * rho1)
    state = lax.while_loop(
        lambda s: mild & (s[0] > RHO) & (s[1] < 100), newton(paired), (rho2, jnp.int32(0))
    )
    lax.while_loop(lambda s: (s[0] > RHO) & (s[1] < 100), newton(precise), state)

    def solved(product):
        inv, system = x[...], m[...]
        a = product(rhs, inv)
        for _ in range(2):
            a = a + product(rhs - precise(a, system), inv)
        return a

    def thirds(v):
        high = v.astype(jnp.bfloat16)
        rest = v - high.astype(jnp.float32)
        mid = rest.astype(jnp.bfloat16)
        return high, mid, (rest - mid.astype(jnp.float32)).astype(jnp.bfloat16)

    def quick():
        ih, il = parts(x[...])

        def apply(v):
            stack = jnp.concatenate(parts(v), axis=0)
            one = matmul(stack, ih)
            return one[:16] + (one[16:] + matmul(stack[:16], il))

        mh, mm, ml = thirds(m[...])
        a = apply(rhs)
        for _ in range(2):
            stack = jnp.concatenate(thirds(a), axis=0)
            one = matmul(stack, mh)
            two = matmul(stack[:32], mm)
            back = one[:16] + ((one[16:32] + two[:16]) + (one[32:] + two[16:] + matmul(stack[:16], ml)))
            a = a + apply(rhs - back)
        return a

    a = lax.cond(mild, quick, lambda: solved(precise))

    aown, aboth = a[:8], a[8:]
    aj, ak = aboth[0:1], aboth[1:2]
    rows = iota((8, LANES), 0)
    lanes = iota((8, LANES), 1)
    flat = rows * LANES + lanes
    nz = noise[...]

    def at(tile, cand):
        return total(jnp.where(flat == cand, tile, 0.0))

    def owned(tile):
        line = jnp.sum(jnp.where(rows == chip // NYX, tile, 0.0), axis=0, keepdims=True)
        return lane_sum(jnp.where(lanes == (chip % NYX) * 8 + rows, line, 0.0))

    sqc, crossc, noisec = owned(sq), owned(cross), owned(nz)
    pa = lane_sum(pown * aown)
    aa = lane_sum(aown * aown)
    pja = lane_sum(aown * pj)
    aja = lane_sum(aown * aj)
    q = sqc - pa
    nrm = sqc - 2.0 * pa + (pa - aa)
    paj = lane_sum(pj * aj)
    qj = at(sq, first) - paj
    big = at(sq, first) - 2.0 * paj + (paj - lane_sum(aj * aj))
    d1 = at(nz, first) + qj
    u = crossc - pja
    e = u - aja
    q2 = q - u * u / d1
    nrm2 = nrm - 2.0 * u * e / d1 + u * u * big / (d1 * d1)
    for row, s in ((0, nrm / (noisec + q)), (1, nrm2 / (noisec + q2))):
        line = jnp.sum(jnp.where(rows == lanes + 4 * core, s, 0.0), axis=0, keepdims=True)
        scores[row : row + 1, :] = line[:, :4]
    uk = at(cross, second) - lane_sum(pj * ak)
    qk = at(sq, second) - lane_sum(pk * ak)
    d2 = at(nz, second) + qk - uk * uk / d1
    r1 = 1.0 / jnp.sqrt(d1)
    r2 = 1.0 / jnp.sqrt(d2)
    ratio = uk / d1

    high = aboth.astype(jnp.bfloat16).astype(jnp.float32)
    rest = aboth - high
    mid = rest.astype(jnp.bfloat16).astype(jnp.float32)
    pieces = jnp.where(rid < 2, high, jnp.where(rid < 4, mid, rest - mid)).astype(jnp.bfloat16)
    copy.wait()
    wide = LANES * NB
    for g in range(dense.shape[0]):
        part = slice(wide * g, wide * (g + 1))
        got = matmul(pieces, fvmem[part, :], ((1,), (1,)))
        applied = got[0:2] + got[2:4] + got[4:6]
        left = dense[g][0:2] - applied
        w1 = left[0:1]
        updates[0:1, part] = w1 * r1
        updates[1:2, part] = (left[1:2] - w1 * ratio) * r2


def finish(mine, theirs, noise, dense, factor, chosen, where):
    local_rows = factor.shape[0]
    vmem = pl.BlockSpec(memory_space=pltpu.VMEM)
    return pl.pallas_call(
        finish_kernel,
        grid_spec=pltpu.PrefetchScalarGridSpec(
            num_scalar_prefetch=2,
            grid=(),
            in_specs=[vmem] * 4 + [pl.BlockSpec(memory_space=pl.ANY)],
            out_specs=[vmem, vmem],
            scratch_shapes=[
                pltpu.VMEM(factor.shape, jnp.bfloat16),
                pltpu.VMEM((R, R), jnp.float32),
                pltpu.VMEM((R, R), jnp.float32),
                pltpu.SemaphoreType.DMA,
            ],
        ),
        out_shape=[
            jax.ShapeDtypeStruct((2, 4), jnp.float32),
            jax.ShapeDtypeStruct((2, local_rows), jnp.float32),
        ],
        compiler_params=pltpu.CompilerParams(vmem_limit_bytes=16 * 2**20),
        name="finish",
    )(in_hbm(chosen), where, mine, theirs, noise, dense, in_hbm(factor))


def swap_cores(x):
    return lax.ppermute(x, "rows_3", [(0, 1), (1, 0)])


def per_device(factor, cand_weights, cand_block, noise, chosen):
    core = lax.axis_index("rows_3").astype(jnp.int32)
    chip = lax.axis_index(("rows_0", "rows_1", "rows_2")).astype(jnp.int32)
    where = jnp.stack([core, chip])
    mine, theirs, dense = local_products(factor, cand_weights, cand_block, chosen, where)
    pair = mine + swap_cores(theirs)
    plane = jnp.sum(lax.all_to_all(pair, YX, 0, 0, tiled=True), axis=0)
    shared = jnp.broadcast_to(plane[None, NZ:], (NZ, 2, 8, LANES))
    line = jnp.concatenate([plane[:NZ, None], shared], axis=1)
    summed = jnp.sum(lax.all_to_all(line, "rows_2", 0, 0, tiled=True), axis=0)
    shared = jnp.broadcast_to(summed[None, 1:], (NYX, 2, 8, LANES))
    shared, own = lax.optimization_barrier((shared, summed[:1]))
    gathered = lax.all_to_all(shared, YX, 0, 0, tiled=True)
    known = jnp.concatenate([gathered.reshape(2 * NYX, 8, LANES), own], axis=0)
    scores, updates = finish(
        known, swap_cores(known), noise.reshape(8, LANES), dense, factor, chosen, where
    )
    return scores, updates


def solution(mesh):
    torus = Mesh(mesh.devices.reshape(4, 4, 8, 2), ROWS)
    return jax.shard_map(
        per_device,
        mesh=torus,
        in_specs=(P(ROWS, None), P(ROWS, None), P(), P(), P()),
        out_specs=(P(None, ROWS), P(None, ROWS)),
        check_vma=False,
    )
```

```python
import jax
import jax.numpy as jnp
from jax import lax
from jax.experimental import pallas as pl
from jax.experimental.pallas import tpu as pltpu
from jax.sharding import Mesh
from jax.sharding import PartitionSpec as P

NB = 4
R = 256
NCAND = 1024
LANES = 128
NYX = 16
NZ = 8
SLOTS = NZ + 2
STEPS = 4
MILD = 1024.0
RHO = 1e-2
ROWS = ("rows_0", "rows_1", "rows_2", "rows_3")
YX = ("rows_0", "rows_1")
HIGHEST = lax.Precision.HIGHEST


def iota(shape, dim):
    return lax.broadcasted_iota(jnp.int32, shape, dim)


def in_hbm(x):
    return pltpu.with_memory_space_constraint(x, pltpu.HBM)


def matmul(a, b, dims=((1,), (0,)), precision=None):
    return lax.dot_general(
        a, b, (dims, ((), ())), preferred_element_type=jnp.float32, precision=precision
    )


def local_kernel(
    chosen, blocks, core, fac, wts, block_row, mine, theirs, dense,
    fwide, acc, gram, sq8, cross8, masks, wsel, pay,
):
    step = pl.program_id(0)
    wrows = wts.shape[0]
    first, second = chosen[0], chosen[1]

    @pl.when(step == 0)
    def _():
        acc[...] = jnp.zeros_like(acc)
        gram[...] = jnp.zeros_like(gram)
        sq8[...] = jnp.zeros_like(sq8)
        cross8[...] = jnp.zeros_like(cross8)
        pay[:, :, NZ:, :, :] = jnp.zeros((2, NYX, 2, 8, LANES), jnp.float32)
        column = jnp.broadcast_to(block_row[...].astype(jnp.float32), (LANES, NCAND)).T
        for b in range(NB):
            masks[b] = jnp.where(column == float(b), 1.0, 0.0).astype(jnp.bfloat16)

    w = wts[...]
    for h in range(2):
        fwide[h] = fac[:, LANES * h : LANES * (h + 1)].astype(jnp.float32)
    turned = w.T
    f = fac[...]
    gram[...] += matmul(f.T, f)
    total = acc[...]
    for b in range(NB):
        fb = jnp.concatenate(
            [fwide[h, pl.ds(b, wrows, stride=NB), :] for h in range(2)], axis=1
        ).astype(jnp.bfloat16)
        mask = masks[b]
        seen = jnp.concatenate(
            [turned[:, LANES * q : LANES * (q + 1)] * mask for q in range(wrows // LANES)], axis=1
        )
        total = total + matmul(seen, fb)
    acc[...] = total
    wf = w.astype(jnp.float32)
    sq8[...] += jnp.sum((wf * wf).reshape(wrows // 8, 8, NCAND), axis=0)
    rows = iota((16, LANES), 0)
    lanes = iota((16, LANES), 1)
    picked = jnp.zeros((16, wrows), jnp.float32)
    for row, cand in ((0, first), (1, second)):
        base = pl.multiple_of((cand // LANES) * LANES, LANES)
        hot = jnp.where((rows == row) & (lanes == cand - base), 1.0, 0.0).astype(jnp.bfloat16)
        picked = picked + matmul(hot, wts[:, pl.ds(base, LANES)], ((1,), (1,)))
    cross8[...] += matmul(picked.astype(jnp.bfloat16), w)[:8]
    for q in range(wrows // LANES):
        wsel[step * (wrows // LANES) + q] = picked[:8, LANES * q : LANES * (q + 1)]

    @pl.when(step == STEPS - 1)
    def _():
        proj = acc[...]
        for h in range(2):
            half = proj[:, LANES * h : LANES * (h + 1)]
            pay[h, :, :NZ, :, :] = half.reshape(NYX, NZ, 8, LANES)
        g = gram[...]
        pay[0, :, NZ, :, :] = g[:LANES, :LANES].reshape(NYX, 8, LANES)
        pay[1, :, NZ, :, :] = g[:LANES, LANES:].reshape(NYX, 8, LANES)
        low = g[LANES:, LANES:].reshape(2, NYX // 2, 8, LANES)
        pay[0, : NYX // 2, NZ + 1, :, :] = low[0]
        pay[1, : NYX // 2, NZ + 1, :, :] = low[1]
        for row, cand in ((0, first), (1, second)):
            line = acc[pl.ds(cand, 1), :]
            for h in range(2):
                pay[0, NYX // 2, NZ + 1, 2 * row + h : 2 * row + h + 1, :] = line[
                    :, LANES * h : LANES * (h + 1)
                ]
        sq = jnp.sum(sq8[...], axis=0, keepdims=True)
        same = block_row[...] == blocks[first]
        cross = jnp.where(same, cross8[0:1, :], 0.0)
        for q in range(NCAND // LANES):
            part = slice(LANES * q, LANES * (q + 1))
            pay[1, NYX // 2, NZ + 1, q : q + 1, :] = sq[:, part]
            pay[1, NYX // 2 + 1, NZ + 1, q : q + 1, :] = cross[:, part]
        mine[...] = pay[core[0]]
        theirs[...] = pay[1 - core[0]]
        wide = LANES * NB
        spread = jnp.where(
            iota((LANES, wide), 0) == iota((LANES, wide), 1) // NB, 1.0, 0.0
        ).astype(jnp.bfloat16)
        groups = wsel.shape[0]
        lines = wsel[...].reshape(groups * 8, LANES).astype(jnp.bfloat16)
        repeated = matmul(lines, spread).reshape(groups, 8, wide)
        row = iota((groups, 8, wide), 1)
        place = iota((groups, 8, wide), 2) % NB
        wanted = jnp.where(row == 0, blocks[first], blocks[second])
        dense[...] = jnp.where(place == wanted, repeated, 0.0)


def local_products(factor, cand_weights, cand_block, chosen, core):
    rows, rank = factor.shape
    wrows = cand_weights.shape[0]
    fstep, wstep = rows // STEPS, wrows // STEPS
    groups = wrows // LANES
    payload = jax.ShapeDtypeStruct((NYX, SLOTS, 8, LANES), jnp.float32)
    return pl.pallas_call(
        local_kernel,
        grid_spec=pltpu.PrefetchScalarGridSpec(
            num_scalar_prefetch=3,
            grid=(STEPS,),
            in_specs=[
                pl.BlockSpec((fstep, rank), lambda i, *_: (i, 0)),
                pl.BlockSpec((wstep, NCAND), lambda i, *_: (i, 0)),
                pl.BlockSpec((1, NCAND), lambda i, *_: (0, 0)),
            ],
            out_specs=[pl.BlockSpec(memory_space=pltpu.VMEM)] * 3,
            scratch_shapes=[
                pltpu.VMEM((2, fstep, LANES), jnp.float32),
                pltpu.VMEM((NCAND, rank), jnp.float32),
                pltpu.VMEM((rank, rank), jnp.float32),
                pltpu.VMEM((8, NCAND), jnp.float32),
                pltpu.VMEM((8, NCAND), jnp.float32),
                pltpu.VMEM((NB, NCAND, LANES), jnp.bfloat16),
                pltpu.VMEM((groups, 8, LANES), jnp.float32),
                pltpu.VMEM((2, NYX, SLOTS, 8, LANES), jnp.float32),
            ],
        ),
        out_shape=[payload, payload, jax.ShapeDtypeStruct((groups, 8, LANES * NB), jnp.float32)],
        compiler_params=pltpu.CompilerParams(
            dimension_semantics=("arbitrary",), vmem_limit_bytes=44 * 2**20
        ),
        name="local",
    )(
        in_hbm(chosen),
        in_hbm(cand_block),
        core,
        in_hbm(factor),
        in_hbm(cand_weights),
        cand_block.reshape(1, NCAND),
    )


def parts(x):
    high = x.astype(jnp.bfloat16)
    return high, (x - high.astype(jnp.float32)).astype(jnp.bfloat16)


def paired(p, q):
    ph, pl_ = parts(p)
    qh, ql = parts(q)
    return matmul(
        jnp.concatenate([ph, pl_, ph], axis=1), jnp.concatenate([qh, qh, ql], axis=0)
    )


def total(x):
    return jnp.sum(jnp.sum(x, axis=1, keepdims=True), axis=0, keepdims=True)


def lane_sum(x):
    return jnp.sum(x, axis=1, keepdims=True)


def finish_kernel(
    chosen, where, mine, theirs, noise, dense, factor, scores, updates,
    fvmem, m, x, sem,
):
    copy = pltpu.make_async_copy(factor, fvmem, sem)
    copy.start()
    core, chip = where[0], where[1]
    first, second = chosen[0], chosen[1]
    own = core == 0
    a_, b_ = mine[...], theirs[...]
    first_half = jnp.where(own, a_, b_)
    second_half = jnp.where(own, b_, a_)
    g0 = first_half[: 2 * NYX].reshape(NYX, 2, 8, LANES)
    g1 = second_half[: 2 * NYX].reshape(NYX, 2, 8, LANES)
    half = NYX // 2
    top = g0[:, 0].reshape(LANES, LANES)
    side = g1[:, 0].reshape(LANES, LANES)
    low = jnp.concatenate([g0[:half, 1], g1[:half, 1]], axis=0).reshape(LANES, LANES)
    diag = iota((LANES, LANES), 0) == iota((LANES, LANES), 1)
    m[:LANES, :LANES] = top + jnp.where(diag, 1.0, 0.0)
    m[:LANES, LANES:] = side
    m[LANES:, :LANES] = side.T
    m[LANES:, LANES:] = low + jnp.where(diag, 1.0, 0.0)
    psel, sq, cross = g0[half, 1], g1[half, 1], g1[half + 1, 1]
    pown = jnp.concatenate([first_half[2 * NYX], second_half[2 * NYX]], axis=1)
    pj = jnp.concatenate([psel[0:1], psel[1:2]], axis=1)
    pk = jnp.concatenate([psel[2:3], psel[3:4]], axis=1)
    rid = iota((8, R), 0)
    pboth = jnp.where(rid >= 6, 0.0, jnp.where(rid % 2 == 0, pj, pk))
    rhs = jnp.concatenate([pown, pboth], axis=0)

    full = m[...]
    reach = jnp.max(jnp.sum(jnp.abs(full), axis=0, keepdims=True))
    mild = reach < MILD
    unit = full * (1.0 / reach)

    def precise(p, q):
        return matmul(p, q, precision=HIGHEST)

    @pl.when(mild)
    def _():
        x[...] = paired(unit, unit)

    @pl.when(jnp.logical_not(mild))
    def _():
        x[...] = precise(unit, unit)

    square = x[...]
    norm = jnp.sqrt(jnp.max(total(square * square)))
    bound = jnp.maximum(reach * jnp.minimum(1.001 * jnp.sqrt(norm), 1.0), 1.0)
    rho0 = (bound - 1.0) / (bound + 1.0)
    alpha = 2.0 / (bound + 1.0)
    grow = alpha * (2.0 / (2.0 - rho0 * rho0))
    rho1 = rho0 * rho0 / (2.0 - rho0 * rho0)
    scale1 = 2.0 / (2.0 - rho1 * rho1)
    eye = jnp.where(iota((R, R), 0) == iota((R, R), 1), 1.0, 0.0)
    start = grow * (2.0 * eye - alpha * full)
    prod1 = (grow * reach) * (2.0 * unit - (alpha * reach) * square)

    def newton(product):
        def body(carry):
            rho, count = carry
            scale = 2.0 / (2.0 - rho * rho)
            now = x[...]
            x[...] = scale * (2.0 * now - product(now, product(m[...], now)))
            return rho * rho / (2.0 - rho * rho), count + 1

        return body

    @pl.when(mild)
    def _():
        x[...] = scale1 * (2.0 * start - paired(start, prod1))

    @pl.when(jnp.logical_not(mild))
    def _():
        x[...] = scale1 * (2.0 * start - precise(start, prod1))

    rho2 = rho1 * rho1 / (2.0 - rho1 * rho1)
    state = lax.while_loop(
        lambda s: mild & (s[0] > RHO) & (s[1] < 100), newton(paired), (rho2, jnp.int32(0))
    )
    lax.while_loop(lambda s: (s[0] > RHO) & (s[1] < 100), newton(precise), state)

    def solved(product):
        inv, system = x[...], m[...]
        a = product(rhs, inv)
        for _ in range(2):
            a = a + product(rhs - precise(a, system), inv)
        return a

    def thirds(v):
        high = v.astype(jnp.bfloat16)
        rest = v - high.astype(jnp.float32)
        mid = rest.astype(jnp.bfloat16)
        return high, mid, (rest - mid.astype(jnp.float32)).astype(jnp.bfloat16)

    def quick():
        ih, il = parts(x[...])

        def apply(v):
            stack = jnp.concatenate(parts(v), axis=0)
            one = matmul(stack, ih)
            return one[:16] + (one[16:] + matmul(stack[:16], il))

        mh, mm, ml = thirds(m[...])
        a = apply(rhs)
        for _ in range(2):
            stack = jnp.concatenate(thirds(a), axis=0)
            one = matmul(stack, mh)
            two = matmul(stack[:32], mm)
            back = one[:16] + ((one[16:32] + two[:16]) + (one[32:] + two[16:] + matmul(stack[:16], ml)))
            a = a + apply(rhs - back)
        return a

    a = lax.cond(mild, quick, lambda: solved(precise))

    aown, aboth = a[:8], a[8:]
    aj, ak = aboth[0:1], aboth[1:2]
    rows = iota((8, LANES), 0)
    lanes = iota((8, LANES), 1)
    flat = rows * LANES + lanes
    nz = noise[...]

    def at(tile, cand):
        return total(jnp.where(flat == cand, tile, 0.0))

    def owned(tile):
        line = jnp.sum(jnp.where(rows == chip // NYX, tile, 0.0), axis=0, keepdims=True)
        return lane_sum(jnp.where(lanes == (chip % NYX) * 8 + rows, line, 0.0))

    sqc, crossc, noisec = owned(sq), owned(cross), owned(nz)
    pa = lane_sum(pown * aown)
    aa = lane_sum(aown * aown)
    pja = lane_sum(aown * pj)
    aja = lane_sum(aown * aj)
    q = sqc - pa
    nrm = sqc - 2.0 * pa + (pa - aa)
    paj = lane_sum(pj * aj)
    qj = at(sq, first) - paj
    big = at(sq, first) - 2.0 * paj + (paj - lane_sum(aj * aj))
    d1 = at(nz, first) + qj
    u = crossc - pja
    e = u - aja
    q2 = q - u * u / d1
    nrm2 = nrm - 2.0 * u * e / d1 + u * u * big / (d1 * d1)
    for row, s in ((0, nrm / (noisec + q)), (1, nrm2 / (noisec + q2))):
        line = jnp.sum(jnp.where(rows == lanes + 4 * core, s, 0.0), axis=0, keepdims=True)
        scores[row : row + 1, :] = line[:, :4]
    uk = at(cross, second) - lane_sum(pj * ak)
    qk = at(sq, second) - lane_sum(pk * ak)
    d2 = at(nz, second) + qk - uk * uk / d1
    r1 = 1.0 / jnp.sqrt(d1)
    r2 = 1.0 / jnp.sqrt(d2)
    ratio = uk / d1

    high = aboth.astype(jnp.bfloat16).astype(jnp.float32)
    rest = aboth - high
    mid = rest.astype(jnp.bfloat16).astype(jnp.float32)
    pieces = jnp.where(rid < 2, high, jnp.where(rid < 4, mid, rest - mid)).astype(jnp.bfloat16)
    copy.wait()
    wide = LANES * NB
    for g in range(dense.shape[0]):
        part = slice(wide * g, wide * (g + 1))
        got = matmul(pieces, fvmem[part, :], ((1,), (1,)))
        applied = got[0:2] + got[2:4] + got[4:6]
        left = dense[g][0:2] - applied
        w1 = left[0:1]
        updates[0:1, part] = w1 * r1
        updates[1:2, part] = (left[1:2] - w1 * ratio) * r2


def finish(mine, theirs, noise, dense, factor, chosen, where):
    local_rows = factor.shape[0]
    vmem = pl.BlockSpec(memory_space=pltpu.VMEM)
    return pl.pallas_call(
        finish_kernel,
        grid_spec=pltpu.PrefetchScalarGridSpec(
            num_scalar_prefetch=2,
            grid=(),
            in_specs=[vmem] * 4 + [pl.BlockSpec(memory_space=pl.ANY)],
            out_specs=[vmem, vmem],
            scratch_shapes=[
                pltpu.VMEM(factor.shape, jnp.bfloat16),
                pltpu.VMEM((R, R), jnp.float32),
                pltpu.VMEM((R, R), jnp.float32),
                pltpu.SemaphoreType.DMA,
            ],
        ),
        out_shape=[
            jax.ShapeDtypeStruct((2, 4), jnp.float32),
            jax.ShapeDtypeStruct((2, local_rows), jnp.float32),
        ],
        compiler_params=pltpu.CompilerParams(vmem_limit_bytes=16 * 2**20),
        name="finish",
    )(in_hbm(chosen), where, mine, theirs, noise, dense, in_hbm(factor))


def swap_cores(x):
    return lax.ppermute(x, "rows_3", [(0, 1), (1, 0)])


def per_device(factor, cand_weights, cand_block, noise, chosen):
    core = lax.axis_index("rows_3").astype(jnp.int32)
    chip = lax.axis_index(("rows_0", "rows_1", "rows_2")).astype(jnp.int32)
    where = jnp.stack([core, chip])
    mine, theirs, dense = local_products(factor, cand_weights, cand_block, chosen, where)
    pair = mine + swap_cores(theirs)
    plane = jnp.sum(lax.all_to_all(pair, YX, 0, 0, tiled=True), axis=0)
    shared = jnp.broadcast_to(plane[None, NZ:], (NZ, 2, 8, LANES))
    line = jnp.concatenate([plane[:NZ, None], shared], axis=1)
    summed = jnp.sum(lax.all_to_all(line, "rows_2", 0, 0, tiled=True), axis=0)
    shared = jnp.broadcast_to(summed[None, 1:], (NYX, 2, 8, LANES))
    shared, own = lax.optimization_barrier((shared, summed[:1]))
    gathered = lax.all_to_all(shared, YX, 0, 0, tiled=True)
    known = jnp.concatenate([gathered.reshape(2 * NYX, 8, LANES), own], axis=0)
    scores, updates = finish(
        known, swap_cores(known), noise.reshape(8, LANES), dense, factor, chosen, where
    )
    return scores, updates


def solution(mesh):
    torus = Mesh(mesh.devices.reshape(4, 4, 8, 2), ROWS)
    return jax.shard_map(
        per_device,
        mesh=torus,
        in_specs=(P(ROWS, None), P(ROWS, None), P(), P(), P()),
        out_specs=(P(None, ROWS), P(None, ROWS)),
        check_vma=False,
    )
```

```python
import jax
import jax.numpy as jnp
from jax import lax
from jax.experimental import pallas as pl
from jax.experimental.pallas import tpu as pltpu
from jax.sharding import Mesh
from jax.sharding import PartitionSpec as P

NB = 4
R = 256
NCAND = 1024
LANES = 128
NYX = 16
NZ = 8
SLOTS = NZ + 2
STEPS = 4
MILD = 1024.0
RHO = 1e-2
ROWS = ("rows_0", "rows_1", "rows_2", "rows_3")
YX = ("rows_0", "rows_1")
HIGHEST = lax.Precision.HIGHEST


def iota(shape, dim):
    return lax.broadcasted_iota(jnp.int32, shape, dim)


def in_hbm(x):
    return pltpu.with_memory_space_constraint(x, pltpu.HBM)


def matmul(a, b, dims=((1,), (0,)), precision=None):
    return lax.dot_general(
        a, b, (dims, ((), ())), preferred_element_type=jnp.float32, precision=precision
    )


def local_kernel(
    chosen, blocks, core, fac, wts, block_row, mine, theirs, dense,
    fwide, acc, gram, sq8, cross8, masks, wsel, pay, turned,
):
    step = pl.program_id(0)
    wrows = wts.shape[0]
    first, second = chosen[0], chosen[1]

    @pl.when(step == 0)
    def _():
        acc[...] = jnp.zeros_like(acc)
        gram[...] = jnp.zeros_like(gram)
        sq8[...] = jnp.zeros_like(sq8)
        cross8[...] = jnp.zeros_like(cross8)
        pay[:, :, NZ:, :, :] = jnp.zeros((2, NYX, 2, 8, LANES), jnp.float32)
        column = jnp.broadcast_to(block_row[...].astype(jnp.float32), (LANES, NCAND)).T
        for b in range(NB):
            masks[b] = jnp.where(column == float(b), 1.0, 0.0).astype(jnp.bfloat16)

    w = wts[...]
    for h in range(2):
        fwide[h] = fac[:, LANES * h : LANES * (h + 1)].astype(jnp.float32)
    turned[...] = w.T
    f = fac[...]
    gram[...] += matmul(f.T, f)
    total = acc[...]
    for b in range(NB):
        fb = jnp.concatenate(
            [fwide[h, pl.ds(b, wrows, stride=NB), :] for h in range(2)], axis=1
        ).astype(jnp.bfloat16)
        mask = masks[b]
        seen = jnp.concatenate(
            [turned[:, LANES * q : LANES * (q + 1)] * mask for q in range(wrows // LANES)], axis=1
        )
        total = total + matmul(seen, fb)
    acc[...] = total
    wf = w.astype(jnp.float32)
    sq8[...] += jnp.sum((wf * wf).reshape(wrows // 8, 8, NCAND), axis=0)
    place = iota((16, wrows), 0)
    picked = jnp.zeros((16, wrows), jnp.float32)
    for row, cand in ((0, first), (1, second)):
        base = pl.multiple_of((cand // 16) * 16, 16)
        near = turned[pl.ds(base, 16), :].astype(jnp.float32)
        line = jnp.sum(jnp.where(place == cand - base, near, 0.0), axis=0, keepdims=True)
        picked = picked + jnp.where(place == row, line, 0.0)
    cross8[...] += matmul(picked.astype(jnp.bfloat16), w)[:8]
    for q in range(wrows // LANES):
        wsel[step * (wrows // LANES) + q] = picked[:8, LANES * q : LANES * (q + 1)]

    @pl.when(step == STEPS - 1)
    def _():
        proj = acc[...]
        for h in range(2):
            half = proj[:, LANES * h : LANES * (h + 1)]
            pay[h, :, :NZ, :, :] = half.reshape(NYX, NZ, 8, LANES)
        g = gram[...]
        pay[0, :, NZ, :, :] = g[:LANES, :LANES].reshape(NYX, 8, LANES)
        pay[1, :, NZ, :, :] = g[:LANES, LANES:].reshape(NYX, 8, LANES)
        low = g[LANES:, LANES:].reshape(2, NYX // 2, 8, LANES)
        pay[0, : NYX // 2, NZ + 1, :, :] = low[0]
        pay[1, : NYX // 2, NZ + 1, :, :] = low[1]
        for row, cand in ((0, first), (1, second)):
            line = acc[pl.ds(cand, 1), :]
            for h in range(2):
                pay[0, NYX // 2, NZ + 1, 2 * row + h : 2 * row + h + 1, :] = line[
                    :, LANES * h : LANES * (h + 1)
                ]
        sq = jnp.sum(sq8[...], axis=0, keepdims=True)
        same = block_row[...] == blocks[first]
        cross = jnp.where(same, cross8[0:1, :], 0.0)
        for q in range(NCAND // LANES):
            part = slice(LANES * q, LANES * (q + 1))
            pay[1, NYX // 2, NZ + 1, q : q + 1, :] = sq[:, part]
            pay[1, NYX // 2 + 1, NZ + 1, q : q + 1, :] = cross[:, part]
        mine[...] = pay[core[0]]
        theirs[...] = pay[1 - core[0]]
        wide = LANES * NB
        spread = jnp.where(
            iota((LANES, wide), 0) == iota((LANES, wide), 1) // NB, 1.0, 0.0
        ).astype(jnp.bfloat16)
        groups = wsel.shape[0]
        lines = wsel[...].reshape(groups * 8, LANES).astype(jnp.bfloat16)
        repeated = matmul(lines, spread).reshape(groups, 8, wide)
        row = iota((groups, 8, wide), 1)
        place = iota((groups, 8, wide), 2) % NB
        wanted = jnp.where(row == 0, blocks[first], blocks[second])
        dense[...] = jnp.where(place == wanted, repeated, 0.0)


def local_products(factor, cand_weights, cand_block, chosen, core):
    rows, rank = factor.shape
    wrows = cand_weights.shape[0]
    fstep, wstep = rows // STEPS, wrows // STEPS
    groups = wrows // LANES
    payload = jax.ShapeDtypeStruct((NYX, SLOTS, 8, LANES), jnp.float32)
    return pl.pallas_call(
        local_kernel,
        grid_spec=pltpu.PrefetchScalarGridSpec(
            num_scalar_prefetch=3,
            grid=(STEPS,),
            in_specs=[
                pl.BlockSpec((fstep, rank), lambda i, *_: (i, 0)),
                pl.BlockSpec((wstep, NCAND), lambda i, *_: (i, 0)),
                pl.BlockSpec((1, NCAND), lambda i, *_: (0, 0)),
            ],
            out_specs=[pl.BlockSpec(memory_space=pltpu.VMEM)] * 3,
            scratch_shapes=[
                pltpu.VMEM((2, fstep, LANES), jnp.float32),
                pltpu.VMEM((NCAND, rank), jnp.float32),
                pltpu.VMEM((rank, rank), jnp.float32),
                pltpu.VMEM((8, NCAND), jnp.float32),
                pltpu.VMEM((8, NCAND), jnp.float32),
                pltpu.VMEM((NB, NCAND, LANES), jnp.bfloat16),
                pltpu.VMEM((groups, 8, LANES), jnp.float32),
                pltpu.VMEM((2, NYX, SLOTS, 8, LANES), jnp.float32),
                pltpu.VMEM((NCAND, wstep), jnp.bfloat16),
            ],
        ),
        out_shape=[payload, payload, jax.ShapeDtypeStruct((groups, 8, LANES * NB), jnp.float32)],
        compiler_params=pltpu.CompilerParams(
            dimension_semantics=("arbitrary",), vmem_limit_bytes=44 * 2**20
        ),
        name="local",
    )(
        in_hbm(chosen),
        in_hbm(cand_block),
        core,
        in_hbm(factor),
        in_hbm(cand_weights),
        cand_block.reshape(1, NCAND),
    )


def parts(x):
    high = x.astype(jnp.bfloat16)
    return high, (x - high.astype(jnp.float32)).astype(jnp.bfloat16)


def paired(p, q):
    ph, pl_ = parts(p)
    qh, ql = parts(q)
    return matmul(
        jnp.concatenate([ph, pl_, ph], axis=1), jnp.concatenate([qh, qh, ql], axis=0)
    )


def total(x):
    return jnp.sum(jnp.sum(x, axis=1, keepdims=True), axis=0, keepdims=True)


def lane_sum(x):
    return jnp.sum(x, axis=1, keepdims=True)


def finish_kernel(
    chosen, where, mine, theirs, noise, dense, factor, scores, updates,
    fvmem, m, x, sem,
):
    copy = pltpu.make_async_copy(factor, fvmem, sem)
    copy.start()
    core, chip = where[0], where[1]
    first, second = chosen[0], chosen[1]
    own = core == 0
    a_, b_ = mine[...], theirs[...]
    first_half = jnp.where(own, a_, b_)
    second_half = jnp.where(own, b_, a_)
    g0 = first_half[: 2 * NYX].reshape(NYX, 2, 8, LANES)
    g1 = second_half[: 2 * NYX].reshape(NYX, 2, 8, LANES)
    half = NYX // 2
    top = g0[:, 0].reshape(LANES, LANES)
    side = g1[:, 0].reshape(LANES, LANES)
    low = jnp.concatenate([g0[:half, 1], g1[:half, 1]], axis=0).reshape(LANES, LANES)
    diag = iota((LANES, LANES), 0) == iota((LANES, LANES), 1)
    m[:LANES, :LANES] = top + jnp.where(diag, 1.0, 0.0)
    m[:LANES, LANES:] = side
    m[LANES:, :LANES] = side.T
    m[LANES:, LANES:] = low + jnp.where(diag, 1.0, 0.0)
    psel, sq, cross = g0[half, 1], g1[half, 1], g1[half + 1, 1]
    pown = jnp.concatenate([first_half[2 * NYX], second_half[2 * NYX]], axis=1)
    pj = jnp.concatenate([psel[0:1], psel[1:2]], axis=1)
    pk = jnp.concatenate([psel[2:3], psel[3:4]], axis=1)
    rid = iota((8, R), 0)
    pboth = jnp.where(rid >= 6, 0.0, jnp.where(rid % 2 == 0, pj, pk))
    rhs = jnp.concatenate([pown, pboth], axis=0)

    full = m[...]
    reach = jnp.max(jnp.sum(jnp.abs(full), axis=0, keepdims=True))
    mild = reach < MILD
    unit = full * (1.0 / reach)

    def precise(p, q):
        return matmul(p, q, precision=HIGHEST)

    @pl.when(mild)
    def _():
        x[...] = paired(unit, unit)

    @pl.when(jnp.logical_not(mild))
    def _():
        x[...] = precise(unit, unit)

    square = x[...]
    norm = jnp.sqrt(jnp.max(total(square * square)))
    bound = jnp.maximum(reach * jnp.minimum(1.001 * jnp.sqrt(norm), 1.0), 1.0)
    rho0 = (bound - 1.0) / (bound + 1.0)
    alpha = 2.0 / (bound + 1.0)
    grow = alpha * (2.0 / (2.0 - rho0 * rho0))
    rho1 = rho0 * rho0 / (2.0 - rho0 * rho0)
    scale1 = 2.0 / (2.0 - rho1 * rho1)
    eye = jnp.where(iota((R, R), 0) == iota((R, R), 1), 1.0, 0.0)
    start = grow * (2.0 * eye - alpha * full)
    prod1 = (grow * reach) * (2.0 * unit - (alpha * reach) * square)

    def newton(product):
        def body(carry):
            rho, count = carry
            scale = 2.0 / (2.0 - rho * rho)
            now = x[...]
            x[...] = scale * (2.0 * now - product(now, product(m[...], now)))
            return rho * rho / (2.0 - rho * rho), count + 1

        return body

    @pl.when(mild)
    def _():
        x[...] = scale1 * (2.0 * start - paired(start, prod1))

    @pl.when(jnp.logical_not(mild))
    def _():
        x[...] = scale1 * (2.0 * start - precise(start, prod1))

    rho2 = rho1 * rho1 / (2.0 - rho1 * rho1)
    state = lax.while_loop(
        lambda s: mild & (s[0] > RHO) & (s[1] < 100), newton(paired), (rho2, jnp.int32(0))
    )
    lax.while_loop(lambda s: (s[0] > RHO) & (s[1] < 100), newton(precise), state)

    def solved(product):
        inv, system = x[...], m[...]
        a = product(rhs, inv)
        for _ in range(2):
            a = a + product(rhs - precise(a, system), inv)
        return a

    def thirds(v):
        high = v.astype(jnp.bfloat16)
        rest = v - high.astype(jnp.float32)
        mid = rest.astype(jnp.bfloat16)
        return high, mid, (rest - mid.astype(jnp.float32)).astype(jnp.bfloat16)

    def quick():
        ih, il = parts(x[...])

        def apply(v):
            stack = jnp.concatenate(parts(v), axis=0)
            one = matmul(stack, ih)
            return one[:16] + (one[16:] + matmul(stack[:16], il))

        mh, mm, ml = thirds(m[...])
        a = apply(rhs)
        for _ in range(2):
            stack = jnp.concatenate(thirds(a), axis=0)
            one = matmul(stack, mh)
            two = matmul(stack[:32], mm)
            back = one[:16] + ((one[16:32] + two[:16]) + (one[32:] + two[16:] + matmul(stack[:16], ml)))
            a = a + apply(rhs - back)
        return a

    a = lax.cond(mild, quick, lambda: solved(precise))

    aown, aboth = a[:8], a[8:]
    aj, ak = aboth[0:1], aboth[1:2]
    rows = iota((8, LANES), 0)
    lanes = iota((8, LANES), 1)
    flat = rows * LANES + lanes
    nz = noise[...]

    def at(tile, cand):
        return total(jnp.where(flat == cand, tile, 0.0))

    def owned(tile):
        line = jnp.sum(jnp.where(rows == chip // NYX, tile, 0.0), axis=0, keepdims=True)
        return lane_sum(jnp.where(lanes == (chip % NYX) * 8 + rows, line, 0.0))

    sqc, crossc, noisec = owned(sq), owned(cross), owned(nz)
    pa = lane_sum(pown * aown)
    aa = lane_sum(aown * aown)
    pja = lane_sum(aown * pj)
    aja = lane_sum(aown * aj)
    q = sqc - pa
    nrm = sqc - 2.0 * pa + (pa - aa)
    paj = lane_sum(pj * aj)
    qj = at(sq, first) - paj
    big = at(sq, first) - 2.0 * paj + (paj - lane_sum(aj * aj))
    d1 = at(nz, first) + qj
    u = crossc - pja
    e = u - aja
    q2 = q - u * u / d1
    nrm2 = nrm - 2.0 * u * e / d1 + u * u * big / (d1 * d1)
    for row, s in ((0, nrm / (noisec + q)), (1, nrm2 / (noisec + q2))):
        line = jnp.sum(jnp.where(rows == lanes + 4 * core, s, 0.0), axis=0, keepdims=True)
        scores[row : row + 1, :] = line[:, :4]
    uk = at(cross, second) - lane_sum(pj * ak)
    qk = at(sq, second) - lane_sum(pk * ak)
    d2 = at(nz, second) + qk - uk * uk / d1
    r1 = 1.0 / jnp.sqrt(d1)
    r2 = 1.0 / jnp.sqrt(d2)
    ratio = uk / d1

    high = aboth.astype(jnp.bfloat16).astype(jnp.float32)
    rest = aboth - high
    mid = rest.astype(jnp.bfloat16).astype(jnp.float32)
    pieces = jnp.where(rid < 2, high, jnp.where(rid < 4, mid, rest - mid)).astype(jnp.bfloat16)
    copy.wait()
    wide = LANES * NB
    for g in range(dense.shape[0]):
        part = slice(wide * g, wide * (g + 1))
        got = matmul(pieces, fvmem[part, :], ((1,), (1,)))
        applied = got[0:2] + got[2:4] + got[4:6]
        left = dense[g][0:2] - applied
        w1 = left[0:1]
        updates[0:1, part] = w1 * r1
        updates[1:2, part] = (left[1:2] - w1 * ratio) * r2


def finish(mine, theirs, noise, dense, factor, chosen, where):
    local_rows = factor.shape[0]
    vmem = pl.BlockSpec(memory_space=pltpu.VMEM)
    return pl.pallas_call(
        finish_kernel,
        grid_spec=pltpu.PrefetchScalarGridSpec(
            num_scalar_prefetch=2,
            grid=(),
            in_specs=[vmem] * 4 + [pl.BlockSpec(memory_space=pl.ANY)],
            out_specs=[vmem, vmem],
            scratch_shapes=[
                pltpu.VMEM(factor.shape, jnp.bfloat16),
                pltpu.VMEM((R, R), jnp.float32),
                pltpu.VMEM((R, R), jnp.float32),
                pltpu.SemaphoreType.DMA,
            ],
        ),
        out_shape=[
            jax.ShapeDtypeStruct((2, 4), jnp.float32),
            jax.ShapeDtypeStruct((2, local_rows), jnp.float32),
        ],
        compiler_params=pltpu.CompilerParams(vmem_limit_bytes=16 * 2**20),
        name="finish",
    )(in_hbm(chosen), where, mine, theirs, noise, dense, in_hbm(factor))


def swap_cores(x):
    return lax.ppermute(x, "rows_3", [(0, 1), (1, 0)])


def per_device(factor, cand_weights, cand_block, noise, chosen):
    core = lax.axis_index("rows_3").astype(jnp.int32)
    chip = lax.axis_index(("rows_0", "rows_1", "rows_2")).astype(jnp.int32)
    where = jnp.stack([core, chip])
    mine, theirs, dense = local_products(factor, cand_weights, cand_block, chosen, where)
    pair = mine + swap_cores(theirs)
    plane = jnp.sum(lax.all_to_all(pair, YX, 0, 0, tiled=True), axis=0)
    shared = jnp.broadcast_to(plane[None, NZ:], (NZ, 2, 8, LANES))
    line = jnp.concatenate([plane[:NZ, None], shared], axis=1)
    summed = jnp.sum(lax.all_to_all(line, "rows_2", 0, 0, tiled=True), axis=0)
    shared = jnp.broadcast_to(summed[None, 1:], (NYX, 2, 8, LANES))
    shared, own = lax.optimization_barrier((shared, summed[:1]))
    gathered = lax.all_to_all(shared, YX, 0, 0, tiled=True)
    known = jnp.concatenate([gathered.reshape(2 * NYX, 8, LANES), own], axis=0)
    scores, updates = finish(
        known, swap_cores(known), noise.reshape(8, LANES), dense, factor, chosen, where
    )
    return scores, updates


def solution(mesh):
    torus = Mesh(mesh.devices.reshape(4, 4, 8, 2), ROWS)
    return jax.shard_map(
        per_device,
        mesh=torus,
        in_specs=(P(ROWS, None), P(ROWS, None), P(), P(), P()),
        out_specs=(P(None, ROWS), P(None, ROWS)),
        check_vma=False,
    )
```
